32 devices in a mesh: gx: 8 (over y, x, core), yz: 4 (over z).
Axes of the slice: x: 2, y: 2, z: 4, core: 2. Of those that a mesh axis runs over, the one named last changes fastest.
Arguments:
- vel: float32 [3, 48, 192, 1024], P(None, 'gx', 'yz'), may hold values from -6 to 6
- q_old: float32 [3, 48, 192, 1024], P(None, 'gx', None, 'yz'), may hold values from -6 to 6
- pressure_guess: float32 [48, 192, 1024], P('gx', None, 'yz'), may hold values from -6 to 6
- shear_shift: int32 [1], replicated, may hold values from 0 to 1023
Outputs:
- vel_next: float32 [3, 48, 192, 1024], P(None, 'gx', 'yz')
- q_next: float32 [3, 48, 192, 1024], P(None, 'gx', None, 'yz')
- pressure: float32 [48, 192, 1024], P('gx', None, 'yz')
The draws below stay inside these ranges and needn't reach their ends.
All inputs are finite; a program needn't handle non-finite values.
Results may differ from the reference program's by a relative error of at most 0.00013.
Values sent between devices are 32-bit elements; how exact they have to be, the bound alone decides.
A program may use at most 128 MiB of HBM per device.

```python
import math
import jax
import jax.numpy as jnp
from jax import lax

NY = 1024
NZ = 192
SWEEPS = 2
NX = 48
N_YZ = 4


def steps_of(rng, dims, cuts, smallest, top_value):
    def one(axis_at, shards_of):
        heights = jax.random.uniform(jax.random.fold_in(jax.random.fold_in(rng, 6), axis_at), (shards_of,), jnp.float32, smallest / len(cuts), top_value / len(cuts))
        return jnp.repeat(jnp.exp(heights), dims[axis_at] // shards_of).reshape((-1,) + (1,) * (len(dims) - axis_at - 1))

    factor_of = one(*cuts[0])
    for cut in cuts[1:]:
        factor_of = factor_of * one(*cut)
    return factor_of


def noise(key, extent, spread, bound, shards=(), kind=jnp.bfloat16):
    array = spread * jax.random.normal(key, extent, jnp.float32)
    if shards:
        array = array * steps_of(key, extent, shards, -0.22, 0.18)
    return jnp.clip(array, -bound, bound).astype(kind)


def setup_inputs(seed: int = 0) -> dict:
    streams_of = jax.random.split(jax.random.key(seed), 5)
    return {
        "vel": noise(streams_of[0], (3, NX, NZ, NY), 1.0, 6.0, ((1, 8), (2, 4)), jnp.float32),
        "q_old": noise(streams_of[1], (3, NX, NZ, NY), 1.0, 6.0, ((1, 8), (3, 4)), jnp.float32),
        "pressure_guess": noise(streams_of[2], (NX, NZ, NY), 1.0, 6.0, ((0, 8), (2, 4)), jnp.float32),
        "shear_shift": jax.random.randint(streams_of[3], (1,), 0, NY).astype(jnp.int32),
    }


highest = lax.Precision.HIGHEST
viscosity = 0.05
time_step = 0.2
keep_weight = -5.0 / 9.0
section_weight = 15.0 / 16.0
shear_param = 1.5
fraction = 0.375

def unpack(packed):
    leading = packed.shape[:-1]
    block_len = NY // (2 * N_YZ)
    viewed = packed.reshape(leading + (N_YZ, 2, block_len))
    return (viewed[..., 0, :].reshape(leading + (NY // 2,)), viewed[..., 1, :].reshape(leading + (NY // 2,)))

def pack(real_part, imag_part):
    leading = real_part.shape[:-1]
    block_len = NY // (2 * N_YZ)
    viewed = jnp.stack([real_part.reshape(leading + (N_YZ, block_len)), imag_part.reshape(leading + (N_YZ, block_len))], axis=-2)
    return viewed.reshape(leading + (NY,))

def x_slice(padded, offset):
    return padded[:, 3 + offset:3 + offset + NX]

def first_diff(padded):
    return (45.0 * (x_slice(padded, 1) - x_slice(padded, -1)) - 9.0 * (x_slice(padded, 2) - x_slice(padded, -2)) + (x_slice(padded, 3) - x_slice(padded, -3))) / 60.0

def second_diff(padded):
    return (2.0 * (x_slice(padded, 3) + x_slice(padded, -3)) - 27.0 * (x_slice(padded, 2) + x_slice(padded, -2)) + 270.0 * (x_slice(padded, 1) + x_slice(padded, -1)) - 490.0 * x_slice(padded, 0)) / 180.0

def rotate(real_part, imag_part, cosine, sine):
    return (real_part * cosine - imag_part * sine, real_part * sine + imag_part * cosine)

def reference(vel, q_old, pressure_guess, shear_shift):
    offset = shear_shift[0]
    tail_rows = vel[:, NX - 3:]
    front_rows = vel[:, :3]
    left_rim = (1.0 - fraction) * jnp.roll(tail_rows, -offset, axis=3) + fraction * jnp.roll(tail_rows, -offset - 1, axis=3)
    right_rim = (1.0 - fraction) * jnp.roll(front_rows, offset, axis=3) + fraction * jnp.roll(front_rows, offset + 1, axis=3)
    padded = jnp.concatenate([left_rim, vel, right_rim], axis=1)
    omega = 2.0 / NX
    xpos = jnp.arange(NX, dtype=jnp.int32).astype(jnp.float32) + 0.5 - NX / 2.0
    background = (-shear_param * omega * xpos)[:, None, None]
    coriolis = jnp.stack([2.0 * omega * vel[1], -(2.0 - shear_param) * omega * vel[0], jnp.zeros_like(vel[0])])
    term_a = -first_diff(padded * padded[0][None]) + viscosity * second_diff(padded) + coriolis
    term_b = -(vel[1] + background)[None] * vel
    term_c = -vel[2][None] * vel
    modes = jnp.arange(NY // 2, dtype=jnp.int32)
    cells_y = jnp.arange(NY, dtype=jnp.int32)
    angle_y = 2.0 * math.pi / NY * (cells_y[:, None] * modes[None, :] % NY).astype(jnp.float32)
    cos_y = jnp.cos(angle_y) / math.sqrt(NY)
    sin_y = jnp.sin(angle_y) / math.sqrt(NY)

    def y_forward(field):
        return (jnp.einsum('cxzy,yk->cxzk', field, cos_y, precision=highest), -jnp.einsum('cxzy,yk->cxzk', field, sin_y, precision=highest))
    ya_re, ya_im = y_forward(term_a)
    yb_re, yb_im = y_forward(term_b)
    yc_re, yc_im = y_forward(term_c)
    yu_re, yu_im = y_forward(vel)
    wave_y = 2.0 * math.pi / NY * modes.astype(jnp.float32)
    w_re = ya_re - wave_y * yb_im - viscosity * (wave_y * wave_y) * yu_re
    w_im = ya_im + wave_y * yb_re - viscosity * (wave_y * wave_y) * yu_im
    cells_z = jnp.arange(NZ, dtype=jnp.int32)
    angle_z = 2.0 * math.pi / NZ * (cells_z[:, None] * cells_z[None, :] % NZ).astype(jnp.float32)
    cos_z = jnp.cos(angle_z) / math.sqrt(NZ)
    sin_z = jnp.sin(angle_z) / math.sqrt(NZ)
    signed_z = jnp.where(cells_z < NZ // 2, cells_z, cells_z - NZ)
    wave_z = (2.0 * math.pi / NZ * signed_z.astype(jnp.float32))[:, None]

    def z_apply(real_part, imag_part, sign):
        cos_re = jnp.einsum('wz,cxzk->cxwk', cos_z, real_part, precision=highest)
        cos_im = jnp.einsum('wz,cxzk->cxwk', cos_z, imag_part, precision=highest)
        sin_re = jnp.einsum('wz,cxzk->cxwk', sin_z, real_part, precision=highest)
        sin_im = jnp.einsum('wz,cxzk->cxwk', sin_z, imag_part, precision=highest)
        return (cos_re + sign * sin_im, cos_im - sign * sin_re)
    zw_re, zw_im = z_apply(w_re, w_im, 1.0)
    zc_re, zc_im = z_apply(yc_re, yc_im, 1.0)
    zu_re, zu_im = z_apply(yu_re, yu_im, 1.0)
    tend_re = zw_re - wave_z * zc_im - viscosity * (wave_z * wave_z) * zu_re
    tend_im = zw_im + wave_z * zc_re - viscosity * (wave_z * wave_z) * zu_im
    edge_angle = 2.0 * math.pi / NY * ((modes * offset % NY).astype(jnp.float32) + fraction * modes.astype(jnp.float32))
    edge_cos = jnp.cos(edge_angle)
    edge_sin = jnp.sin(edge_angle)

    def neighbours(real_part, imag_part):
        low_re, low_im = rotate(real_part[NX - 1:], imag_part[NX - 1:], edge_cos, edge_sin)
        high_re, high_im = rotate(real_part[:1], imag_part[:1], edge_cos, -edge_sin)
        plus_re = jnp.concatenate([real_part[1:], high_re], axis=0)
        plus_im = jnp.concatenate([imag_part[1:], high_im], axis=0)
        minus_re = jnp.concatenate([low_re, real_part[:-1]], axis=0)
        minus_im = jnp.concatenate([low_im, imag_part[:-1]], axis=0)
        return (plus_re, plus_im, minus_re, minus_im)
    xp_re, xp_im, xm_re, xm_im = neighbours(tend_re[0], tend_im[0])
    div_re = 0.5 * (xp_re - xm_re) - wave_y * tend_im[1] - wave_z * tend_im[2]
    div_im = 0.5 * (xp_im - xm_im) + wave_y * tend_re[1] + wave_z * tend_re[2]
    denom = 2.0 + wave_y[None, :] * wave_y[None, :] + wave_z * wave_z
    press_re, press_im = unpack(pressure_guess)
    for sweep_no in range(SWEEPS):
        pp_re, pp_im, pm_re, pm_im = neighbours(press_re, press_im)
        press_re = (pp_re + pm_re - div_re) / denom
        press_im = (pp_im + pm_im - div_im) / denom
    pp_re, pp_im, pm_re, pm_im = neighbours(press_re, press_im)
    grad_re = jnp.stack([0.5 * (pp_re - pm_re), -wave_y * press_im, -wave_z * press_im])
    grad_im = jnp.stack([0.5 * (pp_im - pm_im), wave_y * press_re, wave_z * press_re])
    old_re, old_im = unpack(q_old)
    new_re = keep_weight * old_re + time_step * (tend_re - grad_re)
    new_im = keep_weight * old_im + time_step * (tend_im - grad_im)
    q_next = pack(new_re, new_im)
    back_re, back_im = z_apply(new_re, new_im, -1.0)
    weights = jnp.where(modes == 0, 1.0, 2.0).astype(jnp.float32)
    correction = jnp.einsum('cxzk,yk->cxzy', back_re, cos_y * weights[None, :], precision=highest) - jnp.einsum('cxzk,yk->cxzy', back_im, sin_y * weights[None, :], precision=highest)
    vel_next = vel + section_weight * correction
    return (vel_next, q_next, pack(press_re, press_im))
```

```python
import functools
import math

import jax
import jax.numpy as jnp
import ml_dtypes
import numpy as np
from jax import lax
from jax.experimental import pallas as pl
from jax.experimental.pallas import tpu as pltpu
from jax.sharding import PartitionSpec as P


viscosity = 0.05
time_step = 0.2
keep_weight = -5.0 / 9.0
section_weight = 15.0 / 16.0
shear_param = 1.5
fraction = 0.375

F32 = jnp.float32
BF16 = jnp.bfloat16
VMEM_LIMIT = 62 * 1024 * 1024


def np_parts(matrix):
    high = matrix.astype(np.float32).astype(ml_dtypes.bfloat16)
    low = (matrix - high.astype(np.float64)).astype(np.float32).astype(ml_dtypes.bfloat16)
    return high, low


def parts(x):
    high = x.astype(BF16)
    return high, (x - high.astype(F32)).astype(BF16)


def dot(x, y):
    return jnp.dot(x, y, preferred_element_type=F32)


def dot_t(x, y):
    return lax.dot_general(x, y, (((1,), (1,)), ((), ())), preferred_element_type=F32)


def dot3(a, b, op=dot):
    return op(a[0], b[0]) + (op(a[1], b[0]) + op(a[0], b[1]))


def swap(x):
    return pltpu.roll(x, x.shape[-1] // 2, axis=x.ndim - 1)


def sign_row(cols):
    lane = lax.broadcasted_iota(jnp.int32, (1, cols), 1)
    return jnp.where(lane < cols // 2, -1.0, 1.0).astype(F32)


def take_chunk(v, e, chunks):
    if chunks == 1:
        return v
    w = v.shape[-1] // 2
    lane = lax.broadcasted_iota(jnp.int32, v.shape[:-1] + (w,), v.ndim - 1)
    re, im = v[..., :w], v[..., w:]
    if e == 0:
        return jnp.where(lane < w // 2, re, swap(im))
    return jnp.where(lane < w // 2, swap(re), im)


def merge_chunks(a, b):
    w = a.shape[-1]
    lane = lax.broadcasted_iota(jnp.int32, a.shape, a.ndim - 1)
    re = jnp.where(lane < w // 2, a, swap(b))
    im = jnp.where(lane < w // 2, swap(a), b)
    return re, im


def put(outs, field, value, cw):
    send, keep = outs
    place = pl.program_id(0)
    pairs = pl.num_programs(0) // 2
    _, _, nx, nz, _ = send[0].shape

    def store(refs):
        for e, ref in enumerate(refs):
            ref[0, field] = value[:, e * cw : (e + 1) * cw].reshape(nx, nz, cw)

    pl.when(place < pairs)(lambda: store(send))
    pl.when(place >= pairs)(lambda: store(keep))


def still_fields(order_ref, uz_ref, u_ref, wh_ref, wl_ref, *refs, chunks):
    send, keep = refs[:chunks], refs[chunks : 2 * chunks]
    high, low = refs[2 * chunks :]
    g = order_ref[pl.program_id(0)]
    _, nx, nz, _ = u_ref.shape
    m = nx * nz
    cw = send[0].shape[-1]

    @pl.when(pl.program_id(0) == 0)
    def _():
        for x in range(nx):
            u = u_ref[0, x]
            for at, v in ((x * nz, u), (m + x * nz, -uz_ref[0, x] * u)):
                h, l = parts(v)
                high[at : at + nz] = h
                low[at : at + nz] = l

    out = dot3((high[...], low[...]), (wh_ref[g], wl_ref[g]))
    put((send, keep), 0, out[:m], cw)
    put((send, keep), 1, out[m:], cw)


def moving_field(
    order_ref, shift_ref, mix_ref, back_ref, ux_ref, uy_ref, u_ref, tx_ref, t_ref, fx_ref, f_ref,
    ky_ref, wh_ref, wl_ref, *refs, c, omega, chunks,
):
    us_send, us_keep = refs[:chunks], refs[chunks : 2 * chunks]
    send, keep = refs[2 * chunks : 3 * chunks], refs[3 * chunks : 4 * chunks]
    ghost, high, low = refs[4 * chunks :]
    place = pl.program_id(0)
    pairs = pl.num_programs(0) // 2
    g = order_ref[place]
    _, nx, nz, ny = u_ref.shape
    m = nx * nz
    cw = send[0].shape[-1]

    @pl.when(place == 0)
    def _():
        for i, (tail, front) in enumerate(((tx_ref, fx_ref), (t_ref, f_ref))):
            if i and not c:
                continue
            for j in range(3):
                t = tail[j]
                ghost[i, j] = mix_ref[0] * pltpu.roll(t, shift_ref[0], axis=1) + mix_ref[
                    1
                ] * pltpu.roll(t, shift_ref[1], axis=1)
                f = front[j]
                ghost[i, 3 + j] = mix_ref[2] * pltpu.roll(f, shift_ref[2], axis=1) + mix_ref[
                    3
                ] * pltpu.roll(f, shift_ref[3], axis=1)

        def chunk(i, carry):
            lanes = pl.ds(pl.multiple_of(i * 128, 128), 128)

            def plane(which, x):
                if x < 0:
                    return ghost[which, x + 3, :, lanes]
                if x >= nx:
                    return ghost[which, x - nx + 3, :, lanes]
                return (u_ref if which else ux_ref)[0, x, :, lanes]

            for x in range(nx):
                ux = [plane(0, x + j) for j in range(-3, 4)]
                uy = uy_ref[0, x, :, lanes]
                moving = uy + back_ref[x]
                v = ux if c == 0 else [plane(1, x + j) for j in range(-3, 4)]
                f = [ux[j] * v[j] for j in range(7) if j != 3]
                d1 = (45.0 * (f[3] - f[2]) - 9.0 * (f[4] - f[1]) + (f[5] - f[0])) * (1.0 / 60.0)
                d2 = (
                    2.0 * (v[6] + v[0])
                    - 27.0 * (v[5] + v[1])
                    + 270.0 * (v[4] + v[2])
                    - 490.0 * v[3]
                ) * (1.0 / 180.0)
                a = viscosity * d2 - d1
                if c == 0:
                    a = a + (2.0 * omega) * uy
                if c == 1:
                    a = a - ((2.0 - shear_param) * omega) * ux[3]
                for at, value in ((x * nz, a), (m + x * nz, -moving * v[3])):
                    h, l = parts(value)
                    high[at : at + nz, lanes] = h
                    low[at : at + nz, lanes] = l
            return carry

        lax.fori_loop(0, ny // 128, chunk, 0)

    out = dot3((high[...], low[...]), (wh_ref[g], wl_ref[g]))
    ky = ky_ref[g]
    sign = sign_row(cw)

    def store(old, new):
        for e, (u, ref) in enumerate(zip(old, new)):
            lanes = slice(e * cw, (e + 1) * cw)
            k = ky[:, lanes]
            yu = u[0, 0].reshape(m, cw)
            w = out[:m, lanes] + swap(out[m:, lanes]) * (k * sign) - viscosity * (k * k) * yu
            ref[0, 0] = w.reshape(nx, nz, cw)

    pl.when(place < pairs)(lambda: store(us_send, send))
    pl.when(place >= pairs)(lambda: store(us_keep, keep))


def z_partial(kw_ref, rw_ref, ks_ref, rs_ref, ah_ref, *outs):
    pairs, _, zb, _, cw = kw_ref.shape
    depth = outs[0].shape[1]
    sign = sign_row(cw)
    for at in tuple(range(1, pairs)) + (0,):
        ref = outs[at]
        for x0 in range(0, zb, 2):
            xs = range(x0, min(x0 + 2, zb))
            columns = [
                jnp.concatenate(
                    [
                        kw_ref[at, 0, x], rw_ref[at, 0, x],
                        ks_ref[at, 1, x], rs_ref[at, 1, x],
                        ks_ref[at, 0, x], rs_ref[at, 0, x],
                    ],
                    axis=0,
                )
                for x in xs
            ]
            h, l = parts(jnp.concatenate(columns, axis=-1))
            out = dot(ah_ref[...], jnp.concatenate([h, h, l], axis=0))
            for i, x in enumerate(xs):
                lanes = slice(i * cw, (i + 1) * cw)
                ref[x] = out[:depth, lanes] + swap(out[depth:, lanes]) * sign


def first_sweep(*refs, e, chunks, pieces):
    tx, ty, tz = (refs[c * pieces : (c + 1) * pieces] for c in range(3))
    (
        p_ref, txl_ref, txh_ref, pl_ref, ph_ref, rot_ref, ky_ref, kz_ref, rden_ref,
        div_ref, out_ref, lo_ref, hi_ref,
    ) = refs[3 * pieces :]
    nx, _, cols = div_ref.shape
    sign = sign_row(cols)
    ky = ky_ref[...] * sign
    kz = kz_ref[...] * sign
    rden = rden_ref[...]

    def total(pieces_of, x):
        out = pieces_of[0][x]
        for ref in pieces_of[1:]:
            out = out + ref[x]
        return out

    def rot(v, k):
        return v * rot_ref[2 * k : 2 * k + 1] + swap(v) * rot_ref[2 * k + 1 : 2 * k + 2]

    def guess(v):
        return take_chunk(v, e, chunks)

    for x in range(nx):
        below = total(tx, x - 1) if x else rot(txl_ref[...], 0)
        above = total(tx, x + 1) if x < nx - 1 else rot(txh_ref[...], 1)
        p_below = guess(p_ref[x - 1]) if x else rot(guess(pl_ref[0]), 0)
        p_above = guess(p_ref[x + 1]) if x < nx - 1 else rot(guess(ph_ref[0]), 1)
        div = 0.5 * (above - below) + swap(total(ty, x)) * ky + swap(total(tz, x)) * kz
        div_ref[x] = div
        p = (p_above + p_below - div) * rden
        out_ref[x] = p
        if x == 0:
            lo_ref[0] = p
            lo_ref[1] = -div
        if x == 1:
            lo_ref[1] = lo_ref[1] + p
        if x == nx - 2:
            hi_ref[1] = p
        if x == nx - 1:
            hi_ref[0] = p
            hi_ref[1] = hi_ref[1] - div


def finish(*refs, e, chunks, pieces):
    p1_ref, div_ref, lo_ref, hi_ref, rot_ref, ky_ref, kz_ref, rden_ref, ck_ref = refs[:9]
    refs = refs[9:]
    t_refs = [refs[c * pieces : (c + 1) * pieces] for c in range(3)]
    q_ref, bh_ref, bl_ref = refs[3 * pieces : 3 * pieces + 3]
    refs = refs[3 * pieces + 3 :]
    last = e == chunks - 1
    earlier = chunks > 1 and last
    if earlier:
        q_first, p_first = refs[:2]
        refs = refs[2:]
    qn_ref, p_ref = refs[:2]
    h_refs, press = refs[2:-1], refs[-1]
    nx, depth, cols = p1_ref.shape
    step = pl.program_id(0)
    _, planes, nz, _ = h_refs[0].shape
    sign = sign_row(cols)

    @pl.when(step == 0)
    def _():
        rden = rden_ref[...]

        def rot(v, k):
            return v * rot_ref[2 * k : 2 * k + 1] + swap(v) * rot_ref[2 * k + 1 : 2 * k + 2]

        low = rot(lo_ref[0], 0)
        high = rot(hi_ref[0], 1)
        press[0] = (p1_ref[0] + rot(lo_ref[1], 0)) * rden
        press[nx + 1] = (p1_ref[nx - 1] + rot(hi_ref[1], 1)) * rden
        for i in range(nx):
            below = p1_ref[i - 1] if i else low
            above = p1_ref[i + 1] if i < nx - 1 else high
            press[i + 1] = (above + below - div_ref[i]) * rden

    def leave(ref, at, value, first):
        if earlier:
            re, im = merge_chunks(first, value)
            ref[at + (slice(None), slice(0, cols))] = re
            ref[at + (slice(None), slice(cols, 2 * cols))] = im
        else:
            ref[at] = value

    for i in range(planes):
        x = step * planes + i
        p = press[x + 1]
        leave(p_ref, (i,), p, p_first[i] if earlier else None)
        turned = swap(p) * sign
        grads = (0.5 * (press[x + 2] - press[x]), turned * ky_ref[...], turned * kz_ref[...])
        fresh = []
        for c in range(3):
            t = t_refs[c][0][i]
            for ref in t_refs[c][1:]:
                t = t + ref[i]
            q = keep_weight * take_chunk(q_ref[c, i], e, chunks) + time_step * (t - grads[c])
            leave(qn_ref, (c, i), q, q_first[c, i] if earlier else None)
            fresh.append(q)
        out = dot3((bh_ref[...], bl_ref[...]), parts(jnp.concatenate(fresh, axis=-1)))
        for c in range(3):
            lanes = slice(c * cols, (c + 1) * cols)
            h = (out[:depth, lanes] + swap(out[depth:, lanes]) * sign) * ck_ref[...]
            for k, ref in enumerate(h_refs):
                ref[c, i] = h[k * nz : (k + 1) * nz]


def y_inverse(order_ref, *refs, terms):
    base_ref, wh_ref, wl_ref, out_ref, th, tl = refs[-6:]
    blocks = refs[:-6]
    _, xb, nz, cols = blocks[0].shape

    @pl.when((pl.program_id(0) == 0) & (pl.program_id(1) == 0))
    def _():
        for i, (e, place) in enumerate(terms):
            g = order_ref[place]
            at = slice(i * cols, (i + 1) * cols)
            th[:, at] = wh_ref[g, :, e * cols : (e + 1) * cols]
            tl[:, at] = wl_ref[g, :, e * cols : (e + 1) * cols]

    rows = jnp.concatenate([b[0].reshape(xb * nz, cols) for b in blocks], axis=-1)
    total = dot3(parts(rows), (th[...], tl[...]), dot_t)
    ny = total.shape[-1]
    out_ref[0] = base_ref[0] + section_weight * total.reshape(xb, nz, ny)


def whole(shape):
    return pl.BlockSpec(shape, lambda *_: (0,) * len(shape))


SMEM = pl.BlockSpec(memory_space=pltpu.SMEM)


def shaped(*shape):
    return jax.ShapeDtypeStruct(shape, F32)


def call(body, flops, moved, **kw):
    return pl.pallas_call(
        body,
        compiler_params=pltpu.CompilerParams(vmem_limit_bytes=VMEM_LIMIT),
        cost_estimate=pl.CostEstimate(flops=int(flops), bytes_accessed=int(moved), transcendentals=0),
        **kw,
    )


def section(vel, q_old, pressure_guess, shear_shift):
    _, nx, nz, ny = vel.shape
    depth = q_old.shape[2]
    groups = lax.axis_size("yz")
    slabs = lax.axis_size("gx")
    pairs = groups // 2
    cols = ny // groups
    chunks = 2 if cols % 256 == 0 else 1
    cw = cols // chunks
    half = cw // 2
    block_len = cols // 2
    group_id = lax.axis_index("yz")
    slab_id = lax.axis_index("gx")
    bit = group_id % 2
    pair = group_id // 2
    total_x = nx * slabs
    omega = 2.0 / total_x
    offset = shear_shift[0]
    is_low = slab_id == 0
    is_high = slab_id == slabs - 1

    modes = np.arange(ny // 2).reshape(groups, 1, chunks, half)
    angle = 2.0 * np.pi / ny * (np.arange(ny).reshape(1, ny, 1, 1) * modes % ny)
    table = np.concatenate([np.cos(angle), -np.sin(angle)], axis=-1) / math.sqrt(ny)
    wh, wl = (jnp.asarray(t) for t in np_parts(table.reshape(groups, ny, cols)))
    kz_np = np.fft.fftfreq(depth) * 2.0 * np.pi
    angle_z = 2.0 * np.pi / depth * (np.arange(depth)[:, None] * np.arange(depth)[None, :] % depth)
    cz = np.cos(angle_z) / math.sqrt(depth)
    sz = np.sin(angle_z) / math.sqrt(depth)
    k1 = kz_np[:, None]
    k2 = viscosity * k1 * k1
    forward = np.concatenate(
        [
            np.concatenate([cz, k1 * sz, -k2 * cz], axis=1),
            np.concatenate([-sz, k1 * cz, k2 * sz], axis=1),
        ],
        axis=0,
    )
    paired = groups & (groups - 1) == 0
    paired_cross = pairs & (pairs - 1) == 0

    def partner(i, place):
        return i ^ place if paired else (i + place) % groups

    def across(j, s):
        return j ^ s if paired_cross else (j + s) % pairs

    order = jnp.stack([partner(group_id, place) for place in range(groups)])
    source = order if paired else (group_id - jnp.arange(groups)) % groups
    places = jnp.stack(
        [across(pair, s) * 2 + (1 - bit) for s in range(pairs)]
        + [across(pair, s) * 2 + bit for s in range(pairs)]
    )

    def forward_part(t):
        shaped_t = jnp.asarray(t.reshape(2 * depth, 3, groups, nz))
        rows = jnp.stack([group_id, group_id + 1 - 2 * bit])
        return jnp.take(shaped_t, rows, axis=2).reshape(2 * depth, 3 * 2 * nz)

    def inverse_part(t):
        shaped_t = jnp.asarray(t.reshape(2, groups, nz, depth))
        return jnp.take(shaped_t, order, axis=1).reshape(2 * depth, depth)

    fh, fl = (forward_part(t) for t in np_parts(forward))
    az = jnp.concatenate([fh, fl, fh], axis=1)
    bh, bl = (inverse_part(t) for t in np_parts(np.concatenate([cz, sz], axis=0)))
    ky_half = 2.0 * np.pi / ny * modes
    ky_all = jnp.asarray(
        np.concatenate([ky_half, ky_half], axis=-1).reshape(groups, 1, cols).astype(np.float32)
    )
    kz = jnp.asarray(kz_np.astype(np.float32)[:, None])
    lane = jnp.arange(cw, dtype=jnp.int32)
    sign = jnp.where(lane < half, -1.0, 1.0)
    kys, cks, rdens, rots = [], [], [], []
    for e in range(chunks):
        own = group_id * block_len + e * half + lane % half
        ky = (2.0 * math.pi / ny * own.astype(F32)).reshape(1, cw)
        edge = (
            2.0 * math.pi / ny
            * ((own * offset % ny).astype(F32) + fraction * own.astype(F32))
        )
        cos_e, sin_e = jnp.cos(edge), jnp.sin(edge) * sign
        kys.append(ky)
        cks.append(jnp.where(own == 0, 1.0, 2.0).astype(F32).reshape(1, cw))
        rdens.append(1.0 / (2.0 + ky * ky + kz * kz))
        rots.append(
            jnp.stack(
                [
                    jnp.where(is_low, cos_e, 1.0),
                    jnp.where(is_low, sin_e, 0.0),
                    jnp.where(is_high, cos_e, 1.0),
                    jnp.where(is_high, -sin_e, 0.0),
                ]
            ).astype(F32)
        )
    shifts = jnp.stack([(ny - offset) % ny, (2 * ny - 1 - offset) % ny, offset % ny, (offset + 1) % ny])
    at_edge = jnp.stack([is_low, is_low, is_high, is_high])
    shifts = jnp.where(at_edge, shifts, 0).astype(jnp.int32)
    mix = jnp.where(
        at_edge,
        jnp.array([1.0 - fraction, fraction] * 2, F32),
        jnp.array([1.0, 0.0] * 2, F32),
    )
    xpos = (slab_id * nx + jnp.arange(nx, dtype=jnp.int32)).astype(F32) + 0.5 - total_x / 2.0
    background = -shear_param * omega * xpos

    up = [(i, (i + 1) % slabs) for i in range(slabs)]
    down = [((i + 1) % slabs, i) for i in range(slabs)]
    twins = [(i, i ^ 1) for i in range(groups)]

    def exchange(first, last):
        return lax.ppermute(last, "gx", up), lax.ppermute(first, "gx", down)

    halos = [exchange(vel[0, :3], vel[0, nx - 3 :])]

    m = nx * nz
    y_flops = 2 * m * ny * ny * 3
    half_bytes = 4 * m * ny
    comp = lambda c: pl.BlockSpec((1, nx, nz, ny), lambda p: (c, 0, 0, 0))
    mats = [pltpu.VMEM((2 * m, ny), BF16)] * 2

    def field_specs(fields):
        block = (1, fields, nx, nz, cw)
        send = pl.BlockSpec(block, lambda p: (jnp.minimum(p, pairs - 1), 0, 0, 0, 0))
        keep = pl.BlockSpec(block, lambda p: (jnp.maximum(p - pairs, 0), 0, 0, 0, 0))
        return [send] * chunks + [keep] * chunks

    def still(c):
        return call(
            functools.partial(still_fields, chunks=chunks),
            2 * y_flops,
            4 * half_bytes,
            grid=(groups,),
            in_specs=[SMEM, comp(2), comp(c), whole(wh.shape), whole(wl.shape)],
            out_specs=field_specs(2),
            out_shape=[shaped(pairs, 2, nx, nz, cw)] * (2 * chunks),
            scratch_shapes=mats,
        )(places, vel, vel, wh, wl)

    def moving(c, us):
        return call(
            functools.partial(moving_field, c=c, omega=omega, chunks=chunks),
            2 * y_flops,
            6 * half_bytes,
            grid=(groups,),
            in_specs=[SMEM] * 4
            + [comp(0), comp(1), comp(c)]
            + [whole((3, nz, ny))] * 4
            + [whole(ky_all.shape), whole(wh.shape), whole(wl.shape)]
            + field_specs(1),
            out_specs=field_specs(1),
            out_shape=[shaped(pairs, 1, nx, nz, cw)] * (2 * chunks),
            scratch_shapes=[pltpu.VMEM((2, 6, nz, ny), F32)] + mats,
        )(
            places, shifts, mix, background, vel, vel, vel, halos[0][0], halos[c][0],
            halos[0][1], halos[c][1], ky_all, wh, wl, *us,
        )

    zb = 2 if nx % 2 == 0 else 1
    plane = (depth, cw)

    def z_part(kw, rw, ks, rs):
        outs = call(
            z_partial,
            2 * az.size * pairs * nx * cw,
            10 * half_bytes // groups,
            grid=(nx // zb,),
            in_specs=[
                pl.BlockSpec((pairs, f, zb, nz, cw), lambda x: (0, 0, x, 0, 0)) for f in (1, 1, 2, 2)
            ]
            + [whole(az.shape)],
            out_specs=[pl.BlockSpec((zb,) + plane, lambda x: (x, 0, 0))] * pairs,
            out_shape=[shaped(nx, *plane)] * pairs,
        )(kw, rw, ks, rs, az)
        pieces = [outs[0]]
        for s in range(1, pairs):
            to = [(i, across(i // 2, s) * 2 + i % 2) for i in range(groups)]
            pieces.append(lax.ppermute(outs[s], "yz", to))
        return pieces

    tend = [[None] * 3 for _ in range(chunks)]
    for c in range(3):
        us = still(c)
        if c == 0:
            later, guess, us = lax.optimization_barrier((vel, pressure_guess, us))
            for d in (1, 2):
                halos.append(exchange(later[d, :3], later[d, nx - 3 :]))
            p_low, p_high = exchange(guess[:1], guess[nx - 1 :])
        r_us = [lax.ppermute(us[e], "yz", twins) for e in range(chunks)]
        w = moving(c, us)
        r_w = [lax.ppermute(w[e], "yz", twins) for e in range(chunks)]
        for e in range(chunks):
            tend[e][c] = z_part(w[chunks + e], r_w[e], us[chunks + e], r_us[e])

    fb = 2 if nx % 2 == 0 else 1
    one = pl.BlockSpec((fb,) + plane, lambda x: (x, 0, 0))
    three = pl.BlockSpec((3, fb) + plane, lambda x: (0, x, 0, 0))
    packed = (depth, cols)
    q_done = []
    edges = []
    for e in range(chunks):
        edge_of = lambda x: functools.reduce(jnp.add, [piece[x] for piece in tend[e][0]])
        edges.append(exchange(edge_of(0), edge_of(nx - 1)))
    back = []
    for e in range(chunks):
        flat = [piece for c in range(3) for piece in tend[e][c]]
        t_low, t_high = edges[e]
        div, p1, lo, hi = call(
            functools.partial(first_sweep, e=e, chunks=chunks, pieces=pairs),
            2000 * nx * depth * cw,
            2 * half_bytes,
            out_shape=[shaped(nx, *plane)] * 2 + [shaped(2, *plane)] * 2,
        )(*flat, pressure_guess, t_low, t_high, p_low, p_high, rots[e], kys[e], kz, rdens[e])
        lo_halo, hi_halo = exchange(lo, hi)
        last = e == chunks - 1
        earlier = chunks > 1 and last
        out_plane = packed if last else plane
        consts = (p1, div, lo_halo, hi_halo, rots[e], kys[e], kz, rdens[e], cks[e])
        outs = call(
            functools.partial(finish, e=e, chunks=chunks, pieces=pairs),
            2 * 3 * 3 * nx * 2 * depth * depth * cw,
            3 * half_bytes,
            grid=(nx // fb,),
            in_specs=[whole(v.shape) for v in consts]
            + [one] * len(flat)
            + [pl.BlockSpec((3, fb) + packed, lambda x: (0, x, 0, 0)), whole(bh.shape), whole(bl.shape)]
            + ([three, one] if earlier else []),
            out_specs=[
                pl.BlockSpec((3, fb) + out_plane, lambda x: (0, x, 0, 0)),
                pl.BlockSpec((fb,) + out_plane, lambda x: (x, 0, 0)),
            ]
            + [pl.BlockSpec((3, fb, nz, cw), lambda x: (0, x, 0, 0))] * groups,
            out_shape=[shaped(3, nx, *out_plane), shaped(nx, *out_plane)]
            + [shaped(3, nx, nz, cw)] * groups,
            scratch_shapes=[pltpu.VMEM((nx + 2,) + plane, F32)],
        )(*consts, *flat, q_old, bh, bl, *q_done)
        q_done = list(outs[:2])
        got = [outs[2]]
        for place in range(1, groups):
            to = [(i, partner(i, place)) for i in range(groups)]
            got.append(lax.ppermute(outs[2 + place], "yz", to))
        back.append(got)

    vb = 3 if nx % 3 == 0 else 1
    vel_block = pl.BlockSpec((1, vb, nz, ny), lambda c, x: (c, x, 0, 0))
    batches = [[(e, place) for place in range(groups)] for e in range(chunks - 1)]
    batches += [[(chunks - 1, place) for place in range(2)]]
    batches += [[(chunks - 1, place) for place in range(2, groups)]]
    vel_next = vel
    for terms in batches:
        vel_next = call(
            functools.partial(y_inverse, terms=terms),
            3 * y_flops * len(terms) // (chunks * groups),
            6 * half_bytes,
            grid=(3, nx // vb),
            in_specs=[SMEM]
            + [pl.BlockSpec((1, vb, nz, cw), lambda c, x: (c, x, 0, 0))] * len(terms)
            + [vel_block, whole(wh.shape), whole(wl.shape)],
            out_specs=vel_block,
            out_shape=jax.ShapeDtypeStruct(vel.shape, F32),
            scratch_shapes=[pltpu.VMEM((ny, len(terms) * cw), BF16)] * 2,
        )(source, *[back[e][place] for e, place in terms], vel_next, wh, wl)
    return (vel_next, q_done[0], q_done[1])


def solution(mesh):
    placed = (P(None, "gx", "yz", None), P(None, "gx", None, "yz"), P("gx", None, "yz"), P())
    return jax.shard_map(
        section,
        mesh=mesh,
        in_specs=placed,
        out_specs=(P(None, "gx", "yz", None), P(None, "gx", None, "yz"), P("gx", None, "yz")),
        check_vma=False,
    )
```

```python
import functools
import math

import jax
import jax.numpy as jnp
import ml_dtypes
import numpy as np
from jax import lax
from jax.experimental import pallas as pl
from jax.experimental.pallas import tpu as pltpu
from jax.sharding import PartitionSpec as P


viscosity = 0.05
time_step = 0.2
keep_weight = -5.0 / 9.0
section_weight = 15.0 / 16.0
shear_param = 1.5
fraction = 0.375

F32 = jnp.float32
BF16 = jnp.bfloat16
VMEM_LIMIT = 62 * 1024 * 1024


def np_parts(matrix):
    high = matrix.astype(np.float32).astype(ml_dtypes.bfloat16)
    low = (matrix - high.astype(np.float64)).astype(np.float32).astype(ml_dtypes.bfloat16)
    return high, low


def parts(x):
    high = x.astype(BF16)
    return high, (x - high.astype(F32)).astype(BF16)


def dot(x, y):
    return jnp.dot(x, y, preferred_element_type=F32)


def dot_t(x, y):
    return lax.dot_general(x, y, (((1,), (1,)), ((), ())), preferred_element_type=F32)


def dot3(a, b, op=dot):
    return op(a[0], b[0]) + (op(a[1], b[0]) + op(a[0], b[1]))


def swap(x):
    return pltpu.roll(x, x.shape[-1] // 2, axis=x.ndim - 1)


def sign_row(cols):
    lane = lax.broadcasted_iota(jnp.int32, (1, cols), 1)
    return jnp.where(lane < cols // 2, -1.0, 1.0).astype(F32)


def take_chunk(v, e, chunks):
    if chunks == 1:
        return v
    w = v.shape[-1] // 2
    lane = lax.broadcasted_iota(jnp.int32, v.shape[:-1] + (w,), v.ndim - 1)
    re, im = v[..., :w], v[..., w:]
    if e == 0:
        return jnp.where(lane < w // 2, re, swap(im))
    return jnp.where(lane < w // 2, swap(re), im)


def merge_chunks(a, b):
    w = a.shape[-1]
    lane = lax.broadcasted_iota(jnp.int32, a.shape, a.ndim - 1)
    re = jnp.where(lane < w // 2, a, swap(b))
    im = jnp.where(lane < w // 2, swap(a), b)
    return re, im


def pick(flag, a, b):
    return jnp.where(flag == 1, a, b)


def across(j, s, pairs):
    return j ^ s if pairs & (pairs - 1) == 0 else lax.rem(j + s, pairs)


def partner(i, place, groups):
    return i ^ place if groups & (groups - 1) == 0 else lax.rem(i + place, groups)


def sender(i, place, groups):
    return i ^ place if groups & (groups - 1) == 0 else lax.rem(i + groups - place, groups)


def mode_numbers(group, e, block_len, cols):
    lane = lax.broadcasted_iota(jnp.int32, (1, cols), 1)
    half = cols // 2
    return group * block_len + e * half + jnp.where(lane < half, lane, lane - half)


def y_fields(ids_ref, *refs, c, e, kind, slabs, chunks):
    moves, stays = kind != "still", kind != "moving"
    s = pl.program_id(0)
    pairs = pl.num_programs(0)
    refs = list(refs)
    u_ref = refs.pop(0)
    uz_ref = refs.pop(0) if stays else None
    if moves:
        ux_ref, uy_ref, tx_ref, t_ref, fx_ref, f_ref = refs[:6]
        refs = refs[6:]
    wh_ref, wl_ref = refs[:2]
    refs = refs[2:]
    if kind == "moving":
        us_send, us_keep = refs[:2]
        refs = refs[2:]
    send, keep, high, low = refs[:4]
    ghost = refs[4] if moves else None
    _, nx, nz, ny = u_ref.shape
    m = nx * nz
    cw = send.shape[-1]
    at_u, at_c = (0, m) if stays else (None, None)
    at_a, at_b = (2 * m, 3 * m) if stays else (0, m)
    group = ids_ref[2]
    bit = group & 1
    j = across(group >> 1, s, pairs)
    total_x = nx * slabs
    omega = 2.0 / total_x

    @pl.when(s == 0)
    def _():
        if moves:
            offset, slab = ids_ref[0], ids_ref[1]
            is_low, is_high = slab == 0, slab == slabs - 1
            shifts = (
                jnp.where(is_low, lax.rem(ny - offset, ny), 0),
                jnp.where(is_low, lax.rem(2 * ny - 1 - offset, ny), 0),
                jnp.where(is_high, offset, 0),
                jnp.where(is_high, lax.rem(offset + 1, ny), 0),
            )
            mix = (
                jnp.where(is_low, 1.0 - fraction, 1.0),
                jnp.where(is_low, fraction, 0.0),
                jnp.where(is_high, 1.0 - fraction, 1.0),
                jnp.where(is_high, fraction, 0.0),
            )
            for i, (tail, front) in enumerate(((tx_ref, fx_ref), (t_ref, f_ref))):
                if i and not c:
                    continue
                for d in range(3):
                    t = tail[d]
                    ghost[i, d] = mix[0] * pltpu.roll(t, shifts[0], axis=1) + mix[1] * pltpu.roll(
                        t, shifts[1], axis=1
                    )
                    f = front[d]
                    ghost[i, 3 + d] = mix[2] * pltpu.roll(f, shifts[2], axis=1) + mix[
                        3
                    ] * pltpu.roll(f, shifts[3], axis=1)

        def chunk(i, carry):
            lanes = pl.ds(pl.multiple_of(i * 128, 128), 128)

            def put(at, value):
                h, l = parts(value)
                high[at : at + nz, lanes] = h
                low[at : at + nz, lanes] = l

            def plane(which, x):
                if x < 0:
                    return ghost[which, x + 3, :, lanes]
                if x >= nx:
                    return ghost[which, x - nx + 3, :, lanes]
                return (u_ref if which else ux_ref)[0, x, :, lanes]

            for x in range(nx):
                if stays:
                    u = u_ref[0, x, :, lanes]
                    put(at_u + x * nz, u)
                    put(at_c + x * nz, -uz_ref[0, x, :, lanes] * u)
                if not moves:
                    continue
                place = (ids_ref[1] * nx + x).astype(F32) + (0.5 - total_x / 2.0)
                ux = [plane(0, x + d) for d in range(-3, 4)]
                uy = uy_ref[0, x, :, lanes]
                moving = uy + (-shear_param * omega) * place
                v = ux if c == 0 else [plane(1, x + d) for d in range(-3, 4)]
                f = [ux[d] * v[d] for d in range(7) if d != 3]
                d1 = (45.0 * (f[3] - f[2]) - 9.0 * (f[4] - f[1]) + (f[5] - f[0])) * (1.0 / 60.0)
                d2 = (
                    2.0 * (v[6] + v[0])
                    - 27.0 * (v[5] + v[1])
                    + 270.0 * (v[4] + v[2])
                    - 490.0 * v[3]
                ) * (1.0 / 180.0)
                a = viscosity * d2 - d1
                if c == 0:
                    a = a + (2.0 * omega) * uy
                if c == 1:
                    a = a - ((2.0 - shear_param) * omega) * ux[3]
                put(at_a + x * nz, a)
                put(at_b + x * nz, -moving * v[3])
            return carry

        lax.fori_loop(0, ny // 128, chunk, 0)

    out = dot3((high[...], low[...]), (wh_ref[0, j], wl_ref[0, j]))
    sign = sign_row(cw)
    halves = []
    for b in range(2):
        o = out[:, b * cw : (b + 1) * cw]
        got = [o[at_u : at_u + m], o[at_c : at_c + m]] if stays else []
        if moves:
            modes = mode_numbers(2 * j + b, e, cw * chunks // 2, cw)
            k = (2.0 * math.pi / ny) * modes.astype(F32)
            if stays:
                yu = got[0]
            else:
                sent, kept = us_send[0, 0].reshape(m, cw), us_keep[0, 0].reshape(m, cw)
                yu = pick(bit, kept, sent) if b else pick(bit, sent, kept)
            got.append(
                o[at_a : at_a + m] + swap(o[at_b : at_b + m]) * (k * sign) - viscosity * (k * k) * yu
            )
        halves.append(got)
    for f, (lo, hi) in enumerate(zip(*halves)):
        send[0, f] = pick(bit, lo, hi).reshape(nx, nz, cw)
        keep[0, f] = pick(bit, hi, lo).reshape(nx, nz, cw)


def z_partial(ids_ref, *refs, layout):
    count = 2 * (max(a for a, _ in layout) + 1)
    az_ref, outs = refs[count], refs[count + 1 :]
    pairs, _, zb, _, cw = refs[0].shape
    depth = outs[0].shape[1]
    bit = ids_ref[2] & 1
    matrix = az_ref[ids_ref[2] >> 1]
    sign = sign_row(cw)
    for at in tuple(range(1, pairs)) + (0,):
        ref = outs[at]
        for x0 in range(0, zb, 2):
            xs = range(x0, min(x0 + 2, zb))
            columns = []
            for x in xs:
                rows = []
                for a, f in layout:
                    kept, got = refs[2 * a][at, f, x], refs[2 * a + 1][at, f, x]
                    rows += [pick(bit, got, kept), pick(bit, kept, got)]
                columns.append(jnp.concatenate(rows, axis=0))
            h, l = parts(jnp.concatenate(columns, axis=-1))
            out = dot(matrix, jnp.concatenate([h, h, l], axis=0))
            for i, x in enumerate(xs):
                lanes = slice(i * cw, (i + 1) * cw)
                ref[x] = out[:depth, lanes] + swap(out[depth:, lanes]) * sign


def first_sweep(*refs, e, chunks, pieces):
    tx, ty, tz = (refs[c * pieces : (c + 1) * pieces] for c in range(3))
    (
        p_ref, txl_ref, txh_ref, pl_ref, ph_ref, rot_ref, ky_ref, kz_ref, rden_ref,
        div_ref, out_ref, lo_ref, hi_ref,
    ) = refs[3 * pieces :]
    nx, _, cols = div_ref.shape
    sign = sign_row(cols)
    ky = ky_ref[...] * sign
    kz = kz_ref[...] * sign
    rden = rden_ref[...]

    def total(pieces_of, x):
        out = pieces_of[0][x]
        for ref in pieces_of[1:]:
            out = out + ref[x]
        return out

    def rot(v, k):
        return v * rot_ref[2 * k : 2 * k + 1] + swap(v) * rot_ref[2 * k + 1 : 2 * k + 2]

    def guess(v):
        return take_chunk(v, e, chunks)

    for x in range(nx):
        below = total(tx, x - 1) if x else rot(txl_ref[...], 0)
        above = total(tx, x + 1) if x < nx - 1 else rot(txh_ref[...], 1)
        p_below = guess(p_ref[x - 1]) if x else rot(guess(pl_ref[0]), 0)
        p_above = guess(p_ref[x + 1]) if x < nx - 1 else rot(guess(ph_ref[0]), 1)
        div = 0.5 * (above - below) + swap(total(ty, x)) * ky + swap(total(tz, x)) * kz
        div_ref[x] = div
        p = (p_above + p_below - div) * rden
        out_ref[x] = p
        if x == 0:
            lo_ref[0] = p
            lo_ref[1] = -div
        if x == 1:
            lo_ref[1] = lo_ref[1] + p
        if x == nx - 2:
            hi_ref[1] = p
        if x == nx - 1:
            hi_ref[0] = p
            hi_ref[1] = hi_ref[1] - div


def finish(ids_ref, *refs, e, chunks, pieces, groups):
    p1_ref, div_ref, lo_ref, hi_ref, rot_ref, ky_ref, kz_ref, rden_ref, ck_ref = refs[:9]
    refs = refs[9:]
    t_refs = [refs[c * pieces : (c + 1) * pieces] for c in range(3)]
    q_ref, bh_ref, bl_ref = refs[3 * pieces : 3 * pieces + 3]
    refs = refs[3 * pieces + 3 :]
    last = e == chunks - 1
    earlier = chunks > 1 and last
    if earlier:
        q_first, p_first = refs[:2]
        refs = refs[2:]
    qn_ref, p_ref = refs[:2]
    h_refs, press, hs = refs[2:-2], refs[-2], refs[-1]
    nx, depth, cols = p1_ref.shape
    step = pl.program_id(0)
    _, planes, nz, _ = h_refs[0].shape
    sign = sign_row(cols)

    @pl.when(step == 0)
    def _():
        rden = rden_ref[...]

        def rot(v, k):
            return v * rot_ref[2 * k : 2 * k + 1] + swap(v) * rot_ref[2 * k + 1 : 2 * k + 2]

        low = rot(lo_ref[0], 0)
        high = rot(hi_ref[0], 1)
        press[0] = (p1_ref[0] + rot(lo_ref[1], 0)) * rden
        press[nx + 1] = (p1_ref[nx - 1] + rot(hi_ref[1], 1)) * rden
        for i in range(nx):
            below = p1_ref[i - 1] if i else low
            above = p1_ref[i + 1] if i < nx - 1 else high
            press[i + 1] = (above + below - div_ref[i]) * rden

    def leave(ref, at, value, first):
        if earlier:
            re, im = merge_chunks(first, value)
            ref[at + (slice(None), slice(0, cols))] = re
            ref[at + (slice(None), slice(cols, 2 * cols))] = im
        else:
            ref[at] = value

    for i in range(planes):
        x = step * planes + i
        p = press[x + 1]
        leave(p_ref, (i,), p, p_first[i] if earlier else None)
        turned = swap(p) * sign
        grads = (0.5 * (press[x + 2] - press[x]), turned * ky_ref[...], turned * kz_ref[...])
        fresh = []
        for c in range(3):
            t = t_refs[c][0][i]
            for ref in t_refs[c][1:]:
                t = t + ref[i]
            q = keep_weight * take_chunk(q_ref[c, i], e, chunks) + time_step * (t - grads[c])
            leave(qn_ref, (c, i), q, q_first[c, i] if earlier else None)
            fresh.append(q)
        out = dot3((bh_ref[...], bl_ref[...]), parts(jnp.concatenate(fresh, axis=-1)))
        for c in range(3):
            lanes = slice(c * cols, (c + 1) * cols)
            hs[c] = (out[:depth, lanes] + swap(out[depth:, lanes]) * sign) * ck_ref[...]
            for place, ref in enumerate(h_refs):
                to = partner(ids_ref[2], place, groups)
                ref[c, i] = hs[c, pl.ds(pl.multiple_of(to * nz, 8), nz)]


def y_inverse(ids_ref, *refs, terms, groups):
    base_ref, wh_ref, wl_ref, out_ref, th, tl = refs[-6:]
    blocks = refs[:-6]
    _, xb, nz, cols = blocks[0].shape

    @pl.when((pl.program_id(0) == 0) & (pl.program_id(1) == 0))
    def _():
        for i, (e, place) in enumerate(terms):
            g = sender(ids_ref[2], place, groups)
            at = slice(i * cols, (i + 1) * cols)
            for b in range(2):
                lanes = slice(b * cols, (b + 1) * cols)

                @pl.when(g & 1 == b)
                def _():
                    th[:, at] = wh_ref[e, g >> 1, :, lanes]
                    tl[:, at] = wl_ref[e, g >> 1, :, lanes]

    rows = jnp.concatenate([b[0].reshape(xb * nz, cols) for b in blocks], axis=-1)
    total = dot3(parts(rows), (th[...], tl[...]), dot_t)
    ny = total.shape[-1]
    out_ref[0] = base_ref[0] + section_weight * total.reshape(xb, nz, ny)


def whole(shape):
    return pl.BlockSpec(shape, lambda *_: (0,) * len(shape))


SMEM = pl.BlockSpec(memory_space=pltpu.SMEM)


def shaped(*shape):
    return jax.ShapeDtypeStruct(shape, F32)


def call(body, flops, moved, **kw):
    return pl.pallas_call(
        body,
        compiler_params=pltpu.CompilerParams(vmem_limit_bytes=VMEM_LIMIT),
        cost_estimate=pl.CostEstimate(flops=int(flops), bytes_accessed=int(moved), transcendentals=0),
        **kw,
    )


def section(vel, q_old, pressure_guess, shear_shift):
    _, nx, nz, ny = vel.shape
    depth = q_old.shape[2]
    groups = lax.axis_size("yz")
    slabs = lax.axis_size("gx")
    pairs = groups // 2
    cols = ny // groups
    chunks = 2 if cols % 256 == 0 else 1
    cw = cols // chunks
    half = cw // 2
    block_len = cols // 2
    ids = jnp.stack(
        [shear_shift[0], lax.axis_index("gx").astype(jnp.int32), lax.axis_index("yz").astype(jnp.int32)]
    )

    modes = np.arange(ny // 2).reshape(pairs, 2, chunks, half).transpose(2, 0, 1, 3)[:, :, None]
    angle = 2.0 * np.pi / ny * (np.arange(ny).reshape(1, 1, ny, 1, 1) * modes % ny)
    table = np.concatenate([np.cos(angle), -np.sin(angle)], axis=-1) / math.sqrt(ny)
    wh, wl = (jnp.asarray(t) for t in np_parts(table.reshape(chunks, pairs, ny, 2 * cw)))
    kz_np = np.fft.fftfreq(depth) * 2.0 * np.pi
    angle_z = 2.0 * np.pi / depth * (np.arange(depth)[:, None] * np.arange(depth)[None, :] % depth)
    cz = np.cos(angle_z) / math.sqrt(depth)
    sz = np.sin(angle_z) / math.sqrt(depth)
    k1 = kz_np[:, None]
    k2 = viscosity * k1 * k1
    forward = np.concatenate(
        [
            np.concatenate([cz, k1 * sz, -k2 * cz], axis=1),
            np.concatenate([-sz, k1 * cz, k2 * sz], axis=1),
        ],
        axis=0,
    )
    forward = forward.reshape(2 * depth, 3, pairs, 2 * nz).transpose(2, 0, 1, 3)
    fh, fl = np_parts(forward.reshape(pairs, 2 * depth, 6 * nz))
    az = jnp.asarray(np.concatenate([fh, fl, fh], axis=-1))
    bh, bl = (jnp.asarray(t) for t in np_parts(np.concatenate([cz, sz], axis=0)))
    kz = jnp.asarray(kz_np.astype(np.float32)[:, None])

    up = [(i, (i + 1) % slabs) for i in range(slabs)]
    down = [((i + 1) % slabs, i) for i in range(slabs)]
    twins = [(i, i ^ 1) for i in range(groups)]

    def send(x, axis, to):
        return lax.ppermute(x, axis, to)

    def exchange(first, last):
        return send(last, "gx", up), send(first, "gx", down)

    m = nx * nz
    y_flops = 2 * m * ny * ny * 3
    half_bytes = 4 * m * ny
    comp = lambda c: pl.BlockSpec((1, nx, nz, ny), lambda p: (c, 0, 0, 0))

    def fields(kind, c, e, halos=(), us=()):
        moves, stays = kind != "still", kind != "moving"
        count = 2 * (moves + stays)
        n_out = 2 * stays + moves
        block = lambda f: pl.BlockSpec((1, f, nx, nz, cw), lambda p: (p, 0, 0, 0, 0))
        tables = pl.BlockSpec((1, pairs, ny, 2 * cw), lambda p: (e, 0, 0, 0))
        args, specs = [ids, vel], [SMEM, comp(c)]
        if stays:
            args.append(vel)
            specs.append(comp(2))
        if moves:
            args += [vel, vel, halos[0][0], halos[c][0], halos[0][1], halos[c][1]]
            specs += [comp(0), comp(1)] + [whole((3, nz, ny))] * 4
        args += [wh, wl, *us]
        specs += [tables] * 2 + [block(1)] * len(us)
        return call(
            functools.partial(y_fields, c=c, e=e, kind=kind, slabs=slabs, chunks=chunks),
            count * y_flops // chunks,
            count * half_bytes,
            grid=(pairs,),
            in_specs=specs,
            out_specs=[block(n_out)] * 2,
            out_shape=[shaped(pairs, n_out, nx, nz, cw)] * 2,
            scratch_shapes=[pltpu.VMEM((count * m, ny), BF16)] * 2
            + ([pltpu.VMEM((2, 6, nz, ny), F32)] if moves else []),
        )(*args)

    zb = 2 if nx % 2 == 0 else 1
    plane = (depth, cw)

    def z_part(arrays, layout):
        outs = call(
            functools.partial(z_partial, layout=layout),
            2 * az.size * nx * cw,
            10 * half_bytes // groups,
            grid=(nx // zb,),
            in_specs=[SMEM]
            + [
                pl.BlockSpec((pairs, v.shape[1], zb, nz, cw), lambda x: (0, 0, x, 0, 0))
                for v in arrays
            ]
            + [whole(az.shape)],
            out_specs=[pl.BlockSpec((zb,) + plane, lambda x: (x, 0, 0))] * pairs,
            out_shape=[shaped(nx, *plane)] * pairs,
        )(ids, *arrays, az)
        pieces = [outs[0]]
        for s in range(1, pairs):
            to = [(i, int(across(i // 2, s, pairs)) * 2 + i % 2) for i in range(groups)]
            pieces.append(send(outs[s], "yz", to))
        return pieces

    halos = [exchange(vel[0, :3], vel[0, nx - 3 :])]
    tend = [[None] * 3 for _ in range(chunks)]
    us_send, us_keep = fields("still", 0, 0)
    later, us_send, us_keep = lax.optimization_barrier((vel, us_send, us_keep))
    for d in (1, 2):
        halos.append(exchange(later[d, :3], later[d, nx - 3 :]))
    w_send, w_keep = fields("moving", 0, 0, halos, (us_send, us_keep))
    arrays = (us_keep, send(us_send, "yz", twins), w_keep, send(w_send, "yz", twins))
    tend[0][0] = z_part(arrays, ((1, 0), (0, 1), (0, 0)))
    late = ids
    guess = pressure_guess
    for e in range(chunks):
        for c in range(3):
            if (c, e) == (0, 0):
                continue
            sent, kept = fields("full", c, e, halos)
            if (c, e) == (1, chunks - 1):
                late, guess, sent, kept = lax.optimization_barrier((late, guess, sent, kept))
            arrays = (kept, send(sent, "yz", twins))
            tend[e][c] = z_part(arrays, ((0, 2), (0, 1), (0, 0)))
    p_low, p_high = exchange(guess[:1], guess[nx - 1 :])

    offset, slab_id, group_id = late[0], late[1], late[2]
    is_low = slab_id == 0
    is_high = slab_id == slabs - 1
    lane = jnp.arange(cw, dtype=jnp.int32)
    sign = jnp.where(lane < half, -1.0, 1.0)
    kys, cks, rdens, rots = [], [], [], []
    for e in range(chunks):
        own = group_id * block_len + e * half + lane % half
        ky = (2.0 * math.pi / ny * own.astype(F32)).reshape(1, cw)
        edge = (
            2.0 * math.pi / ny
            * ((own * offset % ny).astype(F32) + fraction * own.astype(F32))
        )
        cos_e, sin_e = jnp.cos(edge), jnp.sin(edge) * sign
        kys.append(ky)
        cks.append(jnp.where(own == 0, 1.0, 2.0).astype(F32).reshape(1, cw))
        rdens.append(1.0 / (2.0 + ky * ky + kz * kz))
        rots.append(
            jnp.stack(
                [
                    jnp.where(is_low, cos_e, 1.0),
                    jnp.where(is_low, sin_e, 0.0),
                    jnp.where(is_high, cos_e, 1.0),
                    jnp.where(is_high, -sin_e, 0.0),
                ]
            ).astype(F32)
        )

    fb = 2 if nx % 2 == 0 else 1
    one = pl.BlockSpec((fb,) + plane, lambda x: (x, 0, 0))
    three = pl.BlockSpec((3, fb) + plane, lambda x: (0, x, 0, 0))
    packed = (depth, cols)
    q_done = []
    edges = []
    for e in range(chunks):
        edge_of = lambda x: functools.reduce(jnp.add, [piece[x] for piece in tend[e][0]])
        edges.append(exchange(edge_of(0), edge_of(nx - 1)))
    back = []
    for e in range(chunks):
        flat = [piece for c in range(3) for piece in tend[e][c]]
        t_low, t_high = edges[e]
        div, p1, lo, hi = call(
            functools.partial(first_sweep, e=e, chunks=chunks, pieces=pairs),
            2000 * nx * depth * cw,
            2 * half_bytes,
            out_shape=[shaped(nx, *plane)] * 2 + [shaped(2, *plane)] * 2,
        )(*flat, pressure_guess, t_low, t_high, p_low, p_high, rots[e], kys[e], kz, rdens[e])
        lo_halo, hi_halo = exchange(lo, hi)
        last = e == chunks - 1
        earlier = chunks > 1 and last
        out_plane = packed if last else plane
        consts = (p1, div, lo_halo, hi_halo, rots[e], kys[e], kz, rdens[e], cks[e])
        outs = call(
            functools.partial(finish, e=e, chunks=chunks, pieces=pairs, groups=groups),
            2 * 3 * 3 * nx * 2 * depth * depth * cw,
            3 * half_bytes,
            grid=(nx // fb,),
            in_specs=[SMEM]
            + [whole(v.shape) for v in consts]
            + [one] * len(flat)
            + [pl.BlockSpec((3, fb) + packed, lambda x: (0, x, 0, 0)), whole(bh.shape), whole(bl.shape)]
            + ([three, one] if earlier else []),
            out_specs=[
                pl.BlockSpec((3, fb) + out_plane, lambda x: (0, x, 0, 0)),
                pl.BlockSpec((fb,) + out_plane, lambda x: (x, 0, 0)),
            ]
            + [pl.BlockSpec((3, fb, nz, cw), lambda x: (0, x, 0, 0))] * groups,
            out_shape=[shaped(3, nx, *out_plane), shaped(nx, *out_plane)]
            + [shaped(3, nx, nz, cw)] * groups,
            scratch_shapes=[pltpu.VMEM((nx + 2,) + plane, F32), pltpu.VMEM((3,) + plane, F32)],
        )(ids, *consts, *flat, q_old, bh, bl, *q_done)
        q_done = list(outs[:2])
        got = [outs[2]]
        for place in range(1, groups):
            to = [(i, int(partner(i, place, groups))) for i in range(groups)]
            got.append(send(outs[2 + place], "yz", to))
        back.append(got)

    vb = 3 if nx % 3 == 0 else 1
    vel_block = pl.BlockSpec((1, vb, nz, ny), lambda c, x: (c, x, 0, 0))
    batches = [[(e, place) for place in range(groups)] for e in range(chunks - 1)]
    batches += [[(chunks - 1, place) for place in range(2)]]
    batches += [[(chunks - 1, place) for place in range(2, groups)]]
    vel_next = vel
    for terms in batches:
        vel_next = call(
            functools.partial(y_inverse, terms=terms, groups=groups),
            3 * y_flops * len(terms) // (chunks * groups),
            6 * half_bytes,
            grid=(3, nx // vb),
            in_specs=[SMEM]
            + [pl.BlockSpec((1, vb, nz, cw), lambda c, x: (c, x, 0, 0))] * len(terms)
            + [vel_block, whole(wh.shape), whole(wl.shape)],
            out_specs=vel_block,
            out_shape=jax.ShapeDtypeStruct(vel.shape, F32),
            scratch_shapes=[pltpu.VMEM((ny, len(terms) * cw), BF16)] * 2,
        )(ids, *[back[e][place] for e, place in terms], vel_next, wh, wl)
    return (vel_next, q_done[0], q_done[1])


def solution(mesh):
    placed = (P(None, "gx", "yz", None), P(None, "gx", None, "yz"), P("gx", None, "yz"), P())
    return jax.shard_map(
        section,
        mesh=mesh,
        in_specs=placed,
        out_specs=(P(None, "gx", "yz", None), P(None, "gx", None, "yz"), P("gx", None, "yz")),
        check_vma=False,
    )
```

```python
import functools
import math

import jax
import jax.numpy as jnp
import ml_dtypes
import numpy as np
from jax import lax
from jax.experimental import pallas as pl
from jax.experimental.pallas import tpu as pltpu
from jax.sharding import PartitionSpec as P


viscosity = 0.05
time_step = 0.2
keep_weight = -5.0 / 9.0
section_weight = 15.0 / 16.0
shear_param = 1.5
fraction = 0.375

F32 = jnp.float32
BF16 = jnp.bfloat16
VMEM_LIMIT = 62 * 1024 * 1024


def np_parts(matrix):
    high = matrix.astype(np.float32).astype(ml_dtypes.bfloat16)
    low = (matrix - high.astype(np.float64)).astype(np.float32).astype(ml_dtypes.bfloat16)
    return high, low


def parts(x):
    high = x.astype(BF16)
    return high, (x - high.astype(F32)).astype(BF16)


def dot(x, y):
    return jnp.dot(x, y, preferred_element_type=F32)


def dot_t(x, y):
    return lax.dot_general(x, y, (((1,), (1,)), ((), ())), preferred_element_type=F32)


def dot3(a, b, op=dot):
    return op(a[0], b[0]) + (op(a[1], b[0]) + op(a[0], b[1]))


def swap(x):
    return pltpu.roll(x, x.shape[-1] // 2, axis=x.ndim - 1)


def sign_row(cols):
    lane = lax.broadcasted_iota(jnp.int32, (1, cols), 1)
    return jnp.where(lane < cols // 2, -1.0, 1.0).astype(F32)


def take_chunk(v, e, chunks):
    if chunks == 1:
        return v
    w = v.shape[-1] // 2
    lane = lax.broadcasted_iota(jnp.int32, v.shape[:-1] + (w,), v.ndim - 1)
    re, im = v[..., :w], v[..., w:]
    if e == 0:
        return jnp.where(lane < w // 2, re, swap(im))
    return jnp.where(lane < w // 2, swap(re), im)


def merge_chunks(a, b):
    w = a.shape[-1]
    lane = lax.broadcasted_iota(jnp.int32, a.shape, a.ndim - 1)
    re = jnp.where(lane < w // 2, a, swap(b))
    im = jnp.where(lane < w // 2, swap(a), b)
    return re, im


def pick(flag, a, b):
    return jnp.where(flag == 1, a, b)


def across(j, s, pairs):
    return j ^ s if pairs & (pairs - 1) == 0 else lax.rem(j + s, pairs)


def partner(i, place, groups):
    return i ^ place if groups & (groups - 1) == 0 else lax.rem(i + place, groups)


def sender(i, place, groups):
    return i ^ place if groups & (groups - 1) == 0 else lax.rem(i + groups - place, groups)


def mode_numbers(group, e, block_len, cols):
    lane = lax.broadcasted_iota(jnp.int32, (1, cols), 1)
    half = cols // 2
    return group * block_len + e * half + jnp.where(lane < half, lane, lane - half)


def y_fields(ids_ref, *refs, c, e, kind, slabs, chunks, direct, u_pairs):
    moves, stays = kind != "still", kind != "moving"
    s = pl.program_id(0)
    pairs = pl.num_programs(0)
    refs = list(refs)
    u_ref = refs.pop(0)
    uz_ref = refs.pop(0) if stays else None
    if moves:
        ux_ref, uy_ref, tx_ref, t_ref, fx_ref, f_ref = refs[:6]
        refs = refs[6:]
    wh_ref, wl_ref = refs[:2]
    refs = refs[2:]
    width = 2 * u_pairs if direct else 2
    outs, (high, low), ghost = refs[:width], refs[width : width + 2], refs[width + 2 :]
    ghost = ghost[0] if moves else None
    _, nx, nz, ny = u_ref.shape
    m = nx * nz
    cw = outs[0].shape[-1]
    at_u, at_c = 0, m
    at_a, at_b = (2 * m, 3 * m) if stays else (m, 2 * m)
    group = ids_ref[2]
    bit = group & 1
    j = across(group >> 1, s, pairs)
    total_x = nx * slabs
    omega = 2.0 / total_x

    @pl.when(s == 0)
    def _():
        if moves:
            offset, slab = ids_ref[0], ids_ref[1]
            is_low, is_high = slab == 0, slab == slabs - 1
            shifts = (
                jnp.where(is_low, lax.rem(ny - offset, ny), 0),
                jnp.where(is_low, lax.rem(2 * ny - 1 - offset, ny), 0),
                jnp.where(is_high, offset, 0),
                jnp.where(is_high, lax.rem(offset + 1, ny), 0),
            )
            mix = (
                jnp.where(is_low, 1.0 - fraction, 1.0),
                jnp.where(is_low, fraction, 0.0),
                jnp.where(is_high, 1.0 - fraction, 1.0),
                jnp.where(is_high, fraction, 0.0),
            )
            for i, (tail, front) in enumerate(((tx_ref, fx_ref), (t_ref, f_ref))):
                if i and not c:
                    continue
                for d in range(3):
                    t = tail[d]
                    ghost[i, d] = mix[0] * pltpu.roll(t, shifts[0], axis=1) + mix[1] * pltpu.roll(
                        t, shifts[1], axis=1
                    )
                    f = front[d]
                    ghost[i, 3 + d] = mix[2] * pltpu.roll(f, shifts[2], axis=1) + mix[
                        3
                    ] * pltpu.roll(f, shifts[3], axis=1)

        def chunk(i, carry):
            lanes = pl.ds(pl.multiple_of(i * 128, 128), 128)

            def put(at, value):
                h, l = parts(value)
                high[at : at + nz, lanes] = h
                low[at : at + nz, lanes] = l

            def plane(which, x):
                if x < 0:
                    return ghost[which, x + 3, :, lanes]
                if x >= nx:
                    return ghost[which, x - nx + 3, :, lanes]
                return (u_ref if which else ux_ref)[0, x, :, lanes]

            for x in range(nx):
                u = u_ref[0, x, :, lanes]
                put(at_u + x * nz, u)
                if stays:
                    put(at_c + x * nz, -uz_ref[0, x, :, lanes] * u)
                if not moves:
                    continue
                place = (ids_ref[1] * nx + x).astype(F32) + (0.5 - total_x / 2.0)
                ux = [plane(0, x + d) for d in range(-3, 4)]
                uy = uy_ref[0, x, :, lanes]
                moving = uy + (-shear_param * omega) * place
                v = ux if c == 0 else [plane(1, x + d) for d in range(-3, 4)]
                f = [ux[d] * v[d] for d in range(7) if d != 3]
                d1 = (45.0 * (f[3] - f[2]) - 9.0 * (f[4] - f[1]) + (f[5] - f[0])) * (1.0 / 60.0)
                d2 = (
                    2.0 * (v[6] + v[0])
                    - 27.0 * (v[5] + v[1])
                    + 270.0 * (v[4] + v[2])
                    - 490.0 * v[3]
                ) * (1.0 / 180.0)
                a = viscosity * d2 - d1
                if c == 0:
                    a = a + (2.0 * omega) * uy
                if c == 1:
                    a = a - ((2.0 - shear_param) * omega) * ux[3]
                put(at_a + x * nz, a)
                put(at_b + x * nz, -moving * v[3])
            return carry

        lax.fori_loop(0, ny // 128, chunk, 0)

    out = dot3((high[...], low[...]), (wh_ref[0, j], wl_ref[0, j]))
    sign = sign_row(cw)
    halves = []
    for b in range(2):
        o = out[:, b * cw : (b + 1) * cw]
        yu = o[at_u : at_u + m]
        got = [yu, o[at_c : at_c + m]] if stays else []
        if moves:
            modes = mode_numbers(2 * j + b, e, cw * chunks // 2, cw)
            k = (2.0 * math.pi / ny) * modes.astype(F32)
            got.append(
                o[at_a : at_a + m] + swap(o[at_b : at_b + m]) * (k * sign) - viscosity * (k * k) * yu
            )
        halves.append(got)

    def store(send, keep):
        for f, (lo, hi) in enumerate(zip(*halves)):
            send[0, f] = pick(bit, lo, hi).reshape(nx, nz, cw)
            keep[0, f] = pick(bit, hi, lo).reshape(nx, nz, cw)

    if not direct:
        store(*outs)
    else:
        for k in range(u_pairs):
            pl.when(s == k)(functools.partial(store, outs[2 * k], outs[2 * k + 1]))


def z_whole(ids_ref, *refs, layout, pairs):
    az_ref, ref = refs[-2:]
    _, _, zb, _, cw = refs[0].shape
    depth = ref.shape[1]
    bit, pair = ids_ref[2] & 1, ids_ref[2] >> 1
    sign = sign_row(cw)
    for x0 in range(0, zb, 2):
        xs = range(x0, min(x0 + 2, zb))
        out = None
        for s in range(pairs):
            columns = []
            for x in xs:
                rows = []
                for a, f in layout:
                    at = 2 * (a * pairs + s)
                    same, other = refs[at][0, f, x], refs[at + 1][0, f, x]
                    rows += [pick(bit, other, same), pick(bit, same, other)]
                columns.append(jnp.concatenate(rows, axis=0))
            h, l = parts(jnp.concatenate(columns, axis=-1))
            matrix = az_ref[sender(pair, s, pairs)]
            term = dot(matrix, jnp.concatenate([h, h, l], axis=0))
            out = term if out is None else out + term
        for i, x in enumerate(xs):
            lanes = slice(i * cw, (i + 1) * cw)
            ref[x] = out[:depth, lanes] + swap(out[depth:, lanes]) * sign


def z_partial(ids_ref, *refs, layout):
    count = 2 * (max(a for a, _ in layout) + 1)
    az_ref, outs = refs[count], refs[count + 1 :]
    pairs, _, zb, _, cw = refs[0].shape
    depth = outs[0].shape[1]
    bit = ids_ref[2] & 1
    matrix = az_ref[ids_ref[2] >> 1]
    sign = sign_row(cw)
    for at in tuple(range(1, pairs)) + (0,):
        ref = outs[at]
        for x0 in range(0, zb, 2):
            xs = range(x0, min(x0 + 2, zb))
            columns = []
            for x in xs:
                rows = []
                for a, f in layout:
                    kept, got = refs[2 * a][at, f, x], refs[2 * a + 1][at, f, x]
                    rows += [pick(bit, got, kept), pick(bit, kept, got)]
                columns.append(jnp.concatenate(rows, axis=0))
            h, l = parts(jnp.concatenate(columns, axis=-1))
            out = dot(matrix, jnp.concatenate([h, h, l], axis=0))
            for i, x in enumerate(xs):
                lanes = slice(i * cw, (i + 1) * cw)
                ref[x] = out[:depth, lanes] + swap(out[depth:, lanes]) * sign


def split(refs, pieces):
    out, at = [], 0
    for n in pieces:
        out.append(refs[at : at + n])
        at += n
    return out


def first_sweep(*refs, e, chunks, pieces):
    tx, ty, tz = split(refs, pieces)
    (
        p_ref, txl_ref, txh_ref, pl_ref, ph_ref, rot_ref, ky_ref, kz_ref, rden_ref,
        div_ref, out_ref, lo_ref, hi_ref,
    ) = refs[sum(pieces) :]
    nx, _, cols = div_ref.shape
    sign = sign_row(cols)
    ky = ky_ref[...] * sign
    kz = kz_ref[...] * sign
    rden = rden_ref[...]

    def total(pieces_of, x):
        out = pieces_of[0][x]
        for ref in pieces_of[1:]:
            out = out + ref[x]
        return out

    def rot(v, k):
        return v * rot_ref[2 * k : 2 * k + 1] + swap(v) * rot_ref[2 * k + 1 : 2 * k + 2]

    def guess(v):
        return take_chunk(v, e, chunks)

    for x in range(nx):
        below = total(tx, x - 1) if x else rot(txl_ref[...], 0)
        above = total(tx, x + 1) if x < nx - 1 else rot(txh_ref[...], 1)
        p_below = guess(p_ref[x - 1]) if x else rot(guess(pl_ref[0]), 0)
        p_above = guess(p_ref[x + 1]) if x < nx - 1 else rot(guess(ph_ref[0]), 1)
        div = 0.5 * (above - below) + swap(total(ty, x)) * ky + swap(total(tz, x)) * kz
        div_ref[x] = div
        p = (p_above + p_below - div) * rden
        out_ref[x] = p
        if x == 0:
            lo_ref[0] = p
            lo_ref[1] = -div
        if x == 1:
            lo_ref[1] = lo_ref[1] + p
        if x == nx - 2:
            hi_ref[1] = p
        if x == nx - 1:
            hi_ref[0] = p
            hi_ref[1] = hi_ref[1] - div


def finish(ids_ref, *refs, e, chunks, pieces, groups):
    p1_ref, div_ref, lo_ref, hi_ref, rot_ref, ky_ref, kz_ref, rden_ref, ck_ref = refs[:9]
    refs = refs[9:]
    t_refs = split(refs, pieces)
    q_ref, bh_ref, bl_ref = refs[sum(pieces) : sum(pieces) + 3]
    refs = refs[sum(pieces) + 3 :]
    last = e == chunks - 1
    earlier = chunks > 1 and last
    if earlier:
        q_first, p_first = refs[:2]
        refs = refs[2:]
    qn_ref, p_ref = refs[:2]
    h_refs, press, hs = refs[2:-2], refs[-2], refs[-1]
    nx, depth, cols = p1_ref.shape
    step = pl.program_id(0)
    _, planes, nz, _ = h_refs[0].shape
    sign = sign_row(cols)

    @pl.when(step == 0)
    def _():
        rden = rden_ref[...]

        def rot(v, k):
            return v * rot_ref[2 * k : 2 * k + 1] + swap(v) * rot_ref[2 * k + 1 : 2 * k + 2]

        low = rot(lo_ref[0], 0)
        high = rot(hi_ref[0], 1)
        press[0] = (p1_ref[0] + rot(lo_ref[1], 0)) * rden
        press[nx + 1] = (p1_ref[nx - 1] + rot(hi_ref[1], 1)) * rden
        for i in range(nx):
            below = p1_ref[i - 1] if i else low
            above = p1_ref[i + 1] if i < nx - 1 else high
            press[i + 1] = (above + below - div_ref[i]) * rden

    def leave(ref, at, value, first):
        if earlier:
            re, im = merge_chunks(first, value)
            ref[at + (slice(None), slice(0, cols))] = re
            ref[at + (slice(None), slice(cols, 2 * cols))] = im
        else:
            ref[at] = value

    for i in range(planes):
        x = step * planes + i
        p = press[x + 1]
        leave(p_ref, (i,), p, p_first[i] if earlier else None)
        turned = swap(p) * sign
        grads = (0.5 * (press[x + 2] - press[x]), turned * ky_ref[...], turned * kz_ref[...])
        fresh = []
        for c in range(3):
            t = t_refs[c][0][i]
            for ref in t_refs[c][1:]:
                t = t + ref[i]
            q = keep_weight * take_chunk(q_ref[c, i], e, chunks) + time_step * (t - grads[c])
            leave(qn_ref, (c, i), q, q_first[c, i] if earlier else None)
            fresh.append(q)
        out = dot3((bh_ref[...], bl_ref[...]), parts(jnp.concatenate(fresh, axis=-1)))
        for c in range(3):
            lanes = slice(c * cols, (c + 1) * cols)
            hs[c] = (out[:depth, lanes] + swap(out[depth:, lanes]) * sign) * ck_ref[...]
            for place, ref in enumerate(h_refs):
                to = partner(ids_ref[2], place, groups)
                ref[c, i] = hs[c, pl.ds(pl.multiple_of(to * nz, 8), nz)]


def y_inverse(ids_ref, *refs, terms, groups):
    base_ref, wh_ref, wl_ref, out_ref, rh, rl, th, tl = refs[-8:]
    blocks = refs[:-8]
    comps, nx, nz, cols = blocks[0].shape
    m = nx * nz

    @pl.when(pl.program_id(0) == 0)
    def _():
        for i, block in enumerate(blocks):
            at = slice(i * cols, (i + 1) * cols)
            for c in range(comps):
                h, l = parts(block[c].reshape(m, cols))
                rh[c * m : (c + 1) * m, at] = h
                rl[c * m : (c + 1) * m, at] = l

    for i, (e, place) in enumerate(terms):
        g = sender(ids_ref[2], place, groups)
        at = slice(i * cols, (i + 1) * cols)
        for b in range(2):
            lanes = slice(b * cols, (b + 1) * cols)

            @pl.when(g & 1 == b)
            def _():
                th[:, at] = wh_ref[e, g >> 1, :, lanes]
                tl[:, at] = wl_ref[e, g >> 1, :, lanes]

    total = dot3((rh[...], rl[...]), (th[...], tl[...]), dot_t)
    out_ref[...] = base_ref[...] + section_weight * total.reshape(out_ref.shape)


def whole(shape):
    return pl.BlockSpec(shape, lambda *_: (0,) * len(shape))


SMEM = pl.BlockSpec(memory_space=pltpu.SMEM)


def shaped(*shape):
    return jax.ShapeDtypeStruct(shape, F32)


def call(body, flops, moved, **kw):
    return pl.pallas_call(
        body,
        compiler_params=pltpu.CompilerParams(vmem_limit_bytes=VMEM_LIMIT),
        cost_estimate=pl.CostEstimate(flops=int(flops), bytes_accessed=int(moved), transcendentals=0),
        **kw,
    )


DIRECT = ((0, 0), (2, 1))


def section(vel, q_old, pressure_guess, shear_shift):
    _, nx, nz, ny = vel.shape
    depth = q_old.shape[2]
    groups = lax.axis_size("yz")
    slabs = lax.axis_size("gx")
    pairs = groups // 2
    cols = ny // groups
    chunks = 2 if cols % 256 == 0 else 1
    cw = cols // chunks
    half = cw // 2
    block_len = cols // 2
    ids = jnp.stack(
        [shear_shift[0], lax.axis_index("gx").astype(jnp.int32), lax.axis_index("yz").astype(jnp.int32)]
    )

    modes = np.arange(ny // 2).reshape(pairs, 2, chunks, half).transpose(2, 0, 1, 3)[:, :, None]
    angle = 2.0 * np.pi / ny * (np.arange(ny).reshape(1, 1, ny, 1, 1) * modes % ny)
    table = np.concatenate([np.cos(angle), -np.sin(angle)], axis=-1) / math.sqrt(ny)
    wh, wl = (jnp.asarray(t) for t in np_parts(table.reshape(chunks, pairs, ny, 2 * cw)))
    kz_np = np.fft.fftfreq(depth) * 2.0 * np.pi
    angle_z = 2.0 * np.pi / depth * (np.arange(depth)[:, None] * np.arange(depth)[None, :] % depth)
    cz = np.cos(angle_z) / math.sqrt(depth)
    sz = np.sin(angle_z) / math.sqrt(depth)
    k1 = kz_np[:, None]
    k2 = viscosity * k1 * k1
    forward = np.concatenate(
        [
            np.concatenate([cz, k1 * sz, -k2 * cz], axis=1),
            np.concatenate([-sz, k1 * cz, k2 * sz], axis=1),
        ],
        axis=0,
    )
    forward = forward.reshape(2 * depth, 3, pairs, 2 * nz).transpose(2, 0, 1, 3)
    fh, fl = np_parts(forward.reshape(pairs, 2 * depth, 6 * nz))
    az = jnp.asarray(np.concatenate([fh, fl, fh], axis=-1))
    bh, bl = (jnp.asarray(t) for t in np_parts(np.concatenate([cz, sz], axis=0)))
    kz = jnp.asarray(kz_np.astype(np.float32)[:, None])

    up = [(i, (i + 1) % slabs) for i in range(slabs)]
    down = [((i + 1) % slabs, i) for i in range(slabs)]
    twins = [(i, i ^ 1) for i in range(groups)]

    def exchange(first, last):
        return lax.ppermute(last, "gx", up), lax.ppermute(first, "gx", down)

    m = nx * nz
    y_flops = 2 * m * ny * ny * 3
    half_bytes = 4 * m * ny
    comp = lambda c: pl.BlockSpec((1, nx, nz, ny), lambda p: (c, 0, 0, 0))

    def fields(kind, c, e, halos=(), direct=False):
        moves, stays = kind != "still", kind != "moving"
        count = {"still": 2, "moving": 3, "full": 4}[kind]
        width = 2 * pairs if direct else 2
        n_out = 2 * stays + moves
        block = lambda f: pl.BlockSpec((1, f, nx, nz, cw), lambda p: (0 if direct else p, 0, 0, 0, 0))
        tables = pl.BlockSpec((1, pairs, ny, 2 * cw), lambda p: (e, 0, 0, 0))
        args, specs = [ids, vel], [SMEM, comp(c)]
        if stays:
            args.append(vel)
            specs.append(comp(2))
        if moves:
            args += [vel, vel, halos[0][0], halos[c][0], halos[0][1], halos[c][1]]
            specs += [comp(0), comp(1)] + [whole((3, nz, ny))] * 4
        args += [wh, wl]
        specs += [tables] * 2
        return call(
            functools.partial(
                y_fields, c=c, e=e, kind=kind, slabs=slabs, chunks=chunks, direct=direct, u_pairs=pairs
            ),
            count * y_flops // chunks,
            count * half_bytes,
            grid=(pairs,),
            in_specs=specs,
            out_specs=[block(n_out)] * width,
            out_shape=[shaped(1 if direct else pairs, n_out, nx, nz, cw)] * width,
            scratch_shapes=[pltpu.VMEM((count * m, ny), BF16)] * 2
            + ([pltpu.VMEM((2, 6, nz, ny), F32)] if moves else []),
        )(*args)

    zb = 2 if nx % 2 == 0 else 1
    plane = (depth, cw)

    def z_part(arrays, layout):
        outs = call(
            functools.partial(z_partial, layout=layout),
            2 * az.size * nx * cw,
            10 * half_bytes // groups,
            grid=(nx // zb,),
            in_specs=[SMEM]
            + [
                pl.BlockSpec((pairs, v.shape[1], zb, nz, cw), lambda x: (0, 0, x, 0, 0))
                for v in arrays
            ]
            + [whole(az.shape)],
            out_specs=[pl.BlockSpec((zb,) + plane, lambda x: (x, 0, 0))] * pairs,
            out_shape=[shaped(nx, *plane)] * pairs,
        )(ids, *arrays, az)
        pieces = [outs[0]]
        for s in range(1, pairs):
            to = [(i, int(across(i // 2, s, pairs)) * 2 + i % 2) for i in range(groups)]
            pieces.append(lax.ppermute(outs[s], "yz", to))
        return pieces

    halos = [exchange(vel[0, :3], vel[0, nx - 3 :])]
    tend = [[None] * 3 for _ in range(chunks)]

    def spread_out(outs):
        got = []
        for s in range(pairs):
            send_s, keep_s = outs[2 * s], outs[2 * s + 1]
            same = [(i, int(across(i // 2, s, pairs)) * 2 + i % 2) for i in range(groups)]
            other = [(i, t ^ 1) for i, t in same]
            got.append(lax.ppermute(keep_s, "yz", same) if s else keep_s)
            got.append(lax.ppermute(send_s, "yz", other))
        return got

    def z_direct(arrays, layout):
        return [
            call(
                functools.partial(z_whole, layout=layout, pairs=pairs),
                2 * az.size * nx * cw,
                10 * half_bytes // groups,
                grid=(nx // zb,),
                in_specs=[SMEM]
                + [
                    pl.BlockSpec((1, v.shape[1], zb, nz, cw), lambda x: (0, 0, x, 0, 0))
                    for v in arrays
                ]
                + [whole(az.shape)],
                out_specs=pl.BlockSpec((zb,) + plane, lambda x: (x, 0, 0)),
                out_shape=shaped(nx, *plane),
            )(ids, *arrays, az)
        ]

    us = fields("still", 0, 0, direct=True)
    later, us = lax.optimization_barrier((vel, us))
    for d in (1, 2):
        halos.append(exchange(later[d, :3], later[d, nx - 3 :]))
    w = fields("moving", 0, 0, halos, direct=True)
    arrays = spread_out(us) + spread_out(w)
    tend[0][0] = z_direct(arrays, ((1, 0), (0, 1), (0, 0)))
    late = ids
    guess = pressure_guess
    for e in range(chunks):
        for c in range(3):
            if tend[e][c]:
                continue
            direct = (c, e) in DIRECT
            outs = fields("full", c, e, halos, direct)
            if (c, e) == (1, chunks - 1):
                late, guess, outs = lax.optimization_barrier((late, guess, outs))
            if direct:
                arrays = spread_out(outs)
                tend[e][c] = z_direct(arrays, ((0, 2), (0, 1), (0, 0)))
            else:
                sent, kept = outs
                arrays = (kept, lax.ppermute(sent, "yz", twins))
                tend[e][c] = z_part(arrays, ((0, 2), (0, 1), (0, 0)))
    p_low, p_high = exchange(guess[:1], guess[nx - 1 :])

    offset, slab_id, group_id = late[0], late[1], late[2]
    is_low = slab_id == 0
    is_high = slab_id == slabs - 1
    lane = jnp.arange(cw, dtype=jnp.int32)
    sign = jnp.where(lane < half, -1.0, 1.0)
    kys, cks, rdens, rots = [], [], [], []
    for e in range(chunks):
        own = group_id * block_len + e * half + lane % half
        ky = (2.0 * math.pi / ny * own.astype(F32)).reshape(1, cw)
        edge = (
            2.0 * math.pi / ny
            * ((own * offset % ny).astype(F32) + fraction * own.astype(F32))
        )
        cos_e, sin_e = jnp.cos(edge), jnp.sin(edge) * sign
        kys.append(ky)
        cks.append(jnp.where(own == 0, 1.0, 2.0).astype(F32).reshape(1, cw))
        rdens.append(1.0 / (2.0 + ky * ky + kz * kz))
        rots.append(
            jnp.stack(
                [
                    jnp.where(is_low, cos_e, 1.0),
                    jnp.where(is_low, sin_e, 0.0),
                    jnp.where(is_high, cos_e, 1.0),
                    jnp.where(is_high, -sin_e, 0.0),
                ]
            ).astype(F32)
        )

    fb = 2 if nx % 2 == 0 else 1
    one = pl.BlockSpec((fb,) + plane, lambda x: (x, 0, 0))
    three = pl.BlockSpec((3, fb) + plane, lambda x: (0, x, 0, 0))
    packed = (depth, cols)
    q_done = []
    edges = []
    for e in range(chunks):
        edge_of = lambda x: functools.reduce(jnp.add, [piece[x] for piece in tend[e][0]])
        edges.append(exchange(edge_of(0), edge_of(nx - 1)))
    back = []
    for e in range(chunks):
        flat = [piece for c in range(3) for piece in tend[e][c]]
        pieces = tuple(len(tend[e][c]) for c in range(3))
        t_low, t_high = edges[e]
        div, p1, lo, hi = call(
            functools.partial(first_sweep, e=e, chunks=chunks, pieces=pieces),
            2000 * nx * depth * cw,
            2 * half_bytes,
            out_shape=[shaped(nx, *plane)] * 2 + [shaped(2, *plane)] * 2,
        )(*flat, pressure_guess, t_low, t_high, p_low, p_high, rots[e], kys[e], kz, rdens[e])
        lo_halo, hi_halo = exchange(lo, hi)
        last = e == chunks - 1
        earlier = chunks > 1 and last
        out_plane = packed if last else plane
        consts = (p1, div, lo_halo, hi_halo, rots[e], kys[e], kz, rdens[e], cks[e])
        outs = call(
            functools.partial(finish, e=e, chunks=chunks, pieces=pieces, groups=groups),
            2 * 3 * 3 * nx * 2 * depth * depth * cw,
            3 * half_bytes,
            grid=(nx // fb,),
            in_specs=[SMEM]
            + [whole(v.shape) for v in consts]
            + [one] * len(flat)
            + [pl.BlockSpec((3, fb) + packed, lambda x: (0, x, 0, 0)), whole(bh.shape), whole(bl.shape)]
            + ([three, one] if earlier else []),
            out_specs=[
                pl.BlockSpec((3, fb) + out_plane, lambda x: (0, x, 0, 0)),
                pl.BlockSpec((fb,) + out_plane, lambda x: (x, 0, 0)),
            ]
            + [pl.BlockSpec((3, fb, nz, cw), lambda x: (0, x, 0, 0))] * groups,
            out_shape=[shaped(3, nx, *out_plane), shaped(nx, *out_plane)]
            + [shaped(3, nx, nz, cw)] * groups,
            scratch_shapes=[pltpu.VMEM((nx + 2,) + plane, F32), pltpu.VMEM((3,) + plane, F32)],
        )(ids, *consts, *flat, q_old, bh, bl, *q_done)
        q_done = list(outs[:2])
        got = [outs[2]]
        for place in range(1, groups):
            to = [(i, int(partner(i, place, groups))) for i in range(groups)]
            got.append(lax.ppermute(outs[2 + place], "yz", to))
        back.append(got)

    yb = ny // 4
    vel_block = pl.BlockSpec((3, nx, nz, yb), lambda i: (0, 0, 0, i))
    table_block = pl.BlockSpec((chunks, pairs, yb, 2 * cw), lambda i: (0, 0, i, 0))
    batches = [[(e, place) for place in range(groups)] for e in range(chunks - 1)]
    batches += [[(chunks - 1, place) for place in range(groups)]]
    vel_next = vel
    for terms in batches:
        vel_next = call(
            functools.partial(y_inverse, terms=terms, groups=groups),
            3 * y_flops * len(terms) // (chunks * groups),
            6 * half_bytes,
            grid=(ny // yb,),
            in_specs=[SMEM]
            + [whole((3, nx, nz, cw))] * len(terms)
            + [vel_block, table_block, table_block],
            out_specs=vel_block,
            out_shape=jax.ShapeDtypeStruct(vel.shape, F32),
            scratch_shapes=[pltpu.VMEM((3 * m, len(terms) * cw), BF16)] * 2
            + [pltpu.VMEM((yb, len(terms) * cw), BF16)] * 2,
        )(ids, *[back[e][place] for e, place in terms], vel_next, wh, wl)
    return (vel_next, q_done[0], q_done[1])


def solution(mesh):
    placed = (P(None, "gx", "yz", None), P(None, "gx", None, "yz"), P("gx", None, "yz"), P())
    return jax.shard_map(
        section,
        mesh=mesh,
        in_specs=placed,
        out_specs=(P(None, "gx", "yz", None), P(None, "gx", None, "yz"), P("gx", None, "yz")),
        check_vma=False,
    )
```

```python
import functools
import math

import jax
import jax.numpy as jnp
import ml_dtypes
import numpy as np
from jax import lax
from jax.experimental import pallas as pl
from jax.experimental.pallas import tpu as pltpu
from jax.sharding import PartitionSpec as P


viscosity = 0.05
time_step = 0.2
keep_weight = -5.0 / 9.0
section_weight = 15.0 / 16.0
shear_param = 1.5
fraction = 0.375

F32 = jnp.float32
BF16 = jnp.bfloat16
VMEM_LIMIT = 62 * 1024 * 1024


def np_parts(matrix):
    high = matrix.astype(np.float32).astype(ml_dtypes.bfloat16)
    low = (matrix - high.astype(np.float64)).astype(np.float32).astype(ml_dtypes.bfloat16)
    return high, low


def parts(x):
    high = x.astype(BF16)
    return high, (x - high.astype(F32)).astype(BF16)


def dot(x, y):
    return jnp.dot(x, y, preferred_element_type=F32)


def dot_t(x, y):
    return lax.dot_general(x, y, (((1,), (1,)), ((), ())), preferred_element_type=F32)


def dot3(a, b, op=dot):
    return op(a[0], b[0]) + (op(a[1], b[0]) + op(a[0], b[1]))


def swap(x):
    return pltpu.roll(x, x.shape[-1] // 2, axis=x.ndim - 1)


def sign_row(cols):
    lane = lax.broadcasted_iota(jnp.int32, (1, cols), 1)
    return jnp.where(lane < cols // 2, -1.0, 1.0).astype(F32)


def take_chunk(v, e, chunks):
    if chunks == 1:
        return v
    w = v.shape[-1] // 2
    lane = lax.broadcasted_iota(jnp.int32, v.shape[:-1] + (w,), v.ndim - 1)
    re, im = v[..., :w], v[..., w:]
    if e == 0:
        return jnp.where(lane < w // 2, re, swap(im))
    return jnp.where(lane < w // 2, swap(re), im)


def merge_chunks(a, b):
    w = a.shape[-1]
    lane = lax.broadcasted_iota(jnp.int32, a.shape, a.ndim - 1)
    re = jnp.where(lane < w // 2, a, swap(b))
    im = jnp.where(lane < w // 2, swap(a), b)
    return re, im


def pick(flag, a, b):
    return jnp.where(flag == 1, a, b)


def across(j, s, pairs):
    return j ^ s if pairs & (pairs - 1) == 0 else lax.rem(j + s, pairs)


def partner(i, place, groups):
    return i ^ place if groups & (groups - 1) == 0 else lax.rem(i + place, groups)


def sender(i, place, groups):
    return i ^ place if groups & (groups - 1) == 0 else lax.rem(i + groups - place, groups)


def mode_numbers(group, e, block_len, cols):
    lane = lax.broadcasted_iota(jnp.int32, (1, cols), 1)
    half = cols // 2
    return group * block_len + e * half + jnp.where(lane < half, lane, lane - half)


def y_fields(ids_ref, *refs, c, e, kind, slabs, chunks, direct, u_pairs):
    moves, stays = kind != "still", kind != "moving"
    s = pl.program_id(0)
    pairs = pl.num_programs(0)
    refs = list(refs)
    u_ref = refs.pop(0)
    uz_ref = refs.pop(0) if stays else None
    if moves:
        ux_ref, uy_ref, tx_ref, t_ref, fx_ref, f_ref = refs[:6]
        refs = refs[6:]
    wh_ref, wl_ref = refs[:2]
    refs = refs[2:]
    width = 2 * u_pairs if direct else 2
    outs, (high, low), ghost = refs[:width], refs[width : width + 2], refs[width + 2 :]
    ghost = ghost[0] if moves else None
    _, nx, nz, ny = u_ref.shape
    m = nx * nz
    cw = outs[0].shape[-1]
    at_u, at_c = 0, m
    at_a, at_b = (2 * m, 3 * m) if stays else (m, 2 * m)
    group = ids_ref[2]
    bit = group & 1
    j = across(group >> 1, s, pairs)
    total_x = nx * slabs
    omega = 2.0 / total_x

    @pl.when(s == 0)
    def _():
        if moves:
            offset, slab = ids_ref[0], ids_ref[1]
            is_low, is_high = slab == 0, slab == slabs - 1
            shifts = (
                jnp.where(is_low, lax.rem(ny - offset, ny), 0),
                jnp.where(is_low, lax.rem(2 * ny - 1 - offset, ny), 0),
                jnp.where(is_high, offset, 0),
                jnp.where(is_high, lax.rem(offset + 1, ny), 0),
            )
            mix = (
                jnp.where(is_low, 1.0 - fraction, 1.0),
                jnp.where(is_low, fraction, 0.0),
                jnp.where(is_high, 1.0 - fraction, 1.0),
                jnp.where(is_high, fraction, 0.0),
            )
            for i, (tail, front) in enumerate(((tx_ref, fx_ref), (t_ref, f_ref))):
                if i and not c:
                    continue
                for d in range(3):
                    t = tail[d]
                    ghost[i, d] = mix[0] * pltpu.roll(t, shifts[0], axis=1) + mix[1] * pltpu.roll(
                        t, shifts[1], axis=1
                    )
                    f = front[d]
                    ghost[i, 3 + d] = mix[2] * pltpu.roll(f, shifts[2], axis=1) + mix[
                        3
                    ] * pltpu.roll(f, shifts[3], axis=1)

        def chunk(i, carry):
            lanes = pl.ds(pl.multiple_of(i * 128, 128), 128)

            def put(at, value):
                h, l = parts(value)
                high[at : at + nz, lanes] = h
                low[at : at + nz, lanes] = l

            def plane(which, x):
                if x < 0:
                    return ghost[which, x + 3, :, lanes]
                if x >= nx:
                    return ghost[which, x - nx + 3, :, lanes]
                return (u_ref if which else ux_ref)[0, x, :, lanes]

            for x in range(nx):
                u = u_ref[0, x, :, lanes]
                put(at_u + x * nz, u)
                if stays:
                    put(at_c + x * nz, -uz_ref[0, x, :, lanes] * u)
                if not moves:
                    continue
                place = (ids_ref[1] * nx + x).astype(F32) + (0.5 - total_x / 2.0)
                ux = [plane(0, x + d) for d in range(-3, 4)]
                uy = uy_ref[0, x, :, lanes]
                moving = uy + (-shear_param * omega) * place
                v = ux if c == 0 else [plane(1, x + d) for d in range(-3, 4)]
                f = [ux[d] * v[d] for d in range(7) if d != 3]
                d1 = (45.0 * (f[3] - f[2]) - 9.0 * (f[4] - f[1]) + (f[5] - f[0])) * (1.0 / 60.0)
                d2 = (
                    2.0 * (v[6] + v[0])
                    - 27.0 * (v[5] + v[1])
                    + 270.0 * (v[4] + v[2])
                    - 490.0 * v[3]
                ) * (1.0 / 180.0)
                a = viscosity * d2 - d1
                if c == 0:
                    a = a + (2.0 * omega) * uy
                if c == 1:
                    a = a - ((2.0 - shear_param) * omega) * ux[3]
                put(at_a + x * nz, a)
                put(at_b + x * nz, -moving * v[3])
            return carry

        lax.fori_loop(0, ny // 128, chunk, 0)

    out = dot3((high[...], low[...]), (wh_ref[0, j], wl_ref[0, j]))
    sign = sign_row(cw)
    halves = []
    for b in range(2):
        o = out[:, b * cw : (b + 1) * cw]
        yu = o[at_u : at_u + m]
        got = [yu, o[at_c : at_c + m]] if stays else []
        if moves:
            modes = mode_numbers(2 * j + b, e, cw * chunks // 2, cw)
            k = (2.0 * math.pi / ny) * modes.astype(F32)
            got.append(
                o[at_a : at_a + m] + swap(o[at_b : at_b + m]) * (k * sign) - viscosity * (k * k) * yu
            )
        halves.append(got)

    def store(send, keep):
        for f, (lo, hi) in enumerate(zip(*halves)):
            send[0, f] = pick(bit, lo, hi).reshape(nx, nz, cw)
            keep[0, f] = pick(bit, hi, lo).reshape(nx, nz, cw)

    if not direct:
        store(*outs)
    else:
        for k in range(u_pairs):
            pl.when(s == k)(functools.partial(store, outs[2 * k], outs[2 * k + 1]))


def z_whole(ids_ref, *refs, layout, pairs):
    az_ref, ref = refs[-2:]
    _, _, zb, _, cw = refs[0].shape
    depth = ref.shape[1]
    bit, pair = ids_ref[2] & 1, ids_ref[2] >> 1
    sign = sign_row(cw)
    for x0 in range(0, zb, 2):
        xs = range(x0, min(x0 + 2, zb))
        out = None
        for s in range(pairs):
            columns = []
            for x in xs:
                rows = []
                for a, f in layout:
                    at = 2 * (a * pairs + s)
                    same, other = refs[at][0, f, x], refs[at + 1][0, f, x]
                    rows += [pick(bit, other, same), pick(bit, same, other)]
                columns.append(jnp.concatenate(rows, axis=0))
            h, l = parts(jnp.concatenate(columns, axis=-1))
            matrix = az_ref[sender(pair, s, pairs)]
            term = dot(matrix, jnp.concatenate([h, h, l], axis=0))
            out = term if out is None else out + term
        for i, x in enumerate(xs):
            lanes = slice(i * cw, (i + 1) * cw)
            ref[x] = out[:depth, lanes] + swap(out[depth:, lanes]) * sign


def z_partial(ids_ref, *refs, layout):
    count = 2 * (max(a for a, _ in layout) + 1)
    az_ref, outs = refs[count], refs[count + 1 :]
    pairs, _, zb, _, cw = refs[0].shape
    depth = outs[0].shape[1]
    bit = ids_ref[2] & 1
    matrix = az_ref[ids_ref[2] >> 1]
    sign = sign_row(cw)
    for at in tuple(range(1, pairs)) + (0,):
        ref = outs[at]
        for x0 in range(0, zb, 2):
            xs = range(x0, min(x0 + 2, zb))
            columns = []
            for x in xs:
                rows = []
                for a, f in layout:
                    kept, got = refs[2 * a][at, f, x], refs[2 * a + 1][at, f, x]
                    rows += [pick(bit, got, kept), pick(bit, kept, got)]
                columns.append(jnp.concatenate(rows, axis=0))
            h, l = parts(jnp.concatenate(columns, axis=-1))
            out = dot(matrix, jnp.concatenate([h, h, l], axis=0))
            for i, x in enumerate(xs):
                lanes = slice(i * cw, (i + 1) * cw)
                ref[x] = out[:depth, lanes] + swap(out[depth:, lanes]) * sign


def split(refs, pieces):
    out, at = [], 0
    for n in pieces:
        out.append(refs[at : at + n])
        at += n
    return out


def first_sweep(*refs, e, chunks, pieces):
    tx, ty, tz = split(refs, pieces)
    (
        p_ref, txl_ref, txh_ref, pl_ref, ph_ref, rot_ref, ky_ref, kz_ref, rden_ref,
        div_ref, out_ref, lo_ref, hi_ref,
    ) = refs[sum(pieces) :]
    nx, _, cols = div_ref.shape
    sign = sign_row(cols)
    ky = ky_ref[...] * sign
    kz = kz_ref[...] * sign
    rden = rden_ref[...]

    def total(pieces_of, x):
        out = pieces_of[0][x]
        for ref in pieces_of[1:]:
            out = out + ref[x]
        return out

    def rot(v, k):
        return v * rot_ref[2 * k : 2 * k + 1] + swap(v) * rot_ref[2 * k + 1 : 2 * k + 2]

    def guess(v):
        return take_chunk(v, e, chunks)

    for x in range(nx):
        below = total(tx, x - 1) if x else rot(txl_ref[...], 0)
        above = total(tx, x + 1) if x < nx - 1 else rot(txh_ref[...], 1)
        p_below = guess(p_ref[x - 1]) if x else rot(guess(pl_ref[0]), 0)
        p_above = guess(p_ref[x + 1]) if x < nx - 1 else rot(guess(ph_ref[0]), 1)
        div = 0.5 * (above - below) + swap(total(ty, x)) * ky + swap(total(tz, x)) * kz
        div_ref[x] = div
        p = (p_above + p_below - div) * rden
        out_ref[x] = p
        if x == 0:
            lo_ref[0] = p
            lo_ref[1] = -div
        if x == 1:
            lo_ref[1] = lo_ref[1] + p
        if x == nx - 2:
            hi_ref[1] = p
        if x == nx - 1:
            hi_ref[0] = p
            hi_ref[1] = hi_ref[1] - div


def finish(ids_ref, *refs, e, chunks, pieces, groups):
    p1_ref, div_ref, lo_ref, hi_ref, rot_ref, ky_ref, kz_ref, rden_ref, ck_ref = refs[:9]
    refs = refs[9:]
    t_refs = split(refs, pieces)
    q_ref, bh_ref, bl_ref = refs[sum(pieces) : sum(pieces) + 3]
    refs = refs[sum(pieces) + 3 :]
    last = e == chunks - 1
    earlier = chunks > 1 and last
    if earlier:
        q_first, p_first = refs[:2]
        refs = refs[2:]
    qn_ref, p_ref = refs[:2]
    h_refs, press, hs = refs[2:-2], refs[-2], refs[-1]
    nx, depth, cols = p1_ref.shape
    step = pl.program_id(0)
    _, planes, nz, _ = h_refs[0].shape
    sign = sign_row(cols)

    @pl.when(step == 0)
    def _():
        rden = rden_ref[...]

        def rot(v, k):
            return v * rot_ref[2 * k : 2 * k + 1] + swap(v) * rot_ref[2 * k + 1 : 2 * k + 2]

        low = rot(lo_ref[0], 0)
        high = rot(hi_ref[0], 1)
        press[0] = (p1_ref[0] + rot(lo_ref[1], 0)) * rden
        press[nx + 1] = (p1_ref[nx - 1] + rot(hi_ref[1], 1)) * rden
        for i in range(nx):
            below = p1_ref[i - 1] if i else low
            above = p1_ref[i + 1] if i < nx - 1 else high
            press[i + 1] = (above + below - div_ref[i]) * rden

    def leave(ref, at, value, first):
        if earlier:
            re, im = merge_chunks(first, value)
            ref[at + (slice(None), slice(0, cols))] = re
            ref[at + (slice(None), slice(cols, 2 * cols))] = im
        else:
            ref[at] = value

    for i in range(planes):
        x = step * planes + i
        p = press[x + 1]
        leave(p_ref, (i,), p, p_first[i] if earlier else None)
        turned = swap(p) * sign
        grads = (0.5 * (press[x + 2] - press[x]), turned * ky_ref[...], turned * kz_ref[...])
        fresh = []
        for c in range(3):
            t = t_refs[c][0][i]
            for ref in t_refs[c][1:]:
                t = t + ref[i]
            q = keep_weight * take_chunk(q_ref[c, i], e, chunks) + time_step * (t - grads[c])
            leave(qn_ref, (c, i), q, q_first[c, i] if earlier else None)
            fresh.append(q)
        out = dot3((bh_ref[...], bl_ref[...]), parts(jnp.concatenate(fresh, axis=-1)))
        for c in range(3):
            lanes = slice(c * cols, (c + 1) * cols)
            hs[c] = (out[:depth, lanes] + swap(out[depth:, lanes]) * sign) * ck_ref[...]
            for place, ref in enumerate(h_refs):
                to = partner(ids_ref[2], place, groups)
                ref[c, i] = hs[c, pl.ds(pl.multiple_of(to * nz, 8), nz)]


def y_inverse(ids_ref, *refs, terms, groups):
    base_ref, wh_ref, wl_ref, out_ref, rh, rl, th, tl = refs[-8:]
    blocks = refs[:-8]
    comps, nx, nz, cols = blocks[0].shape
    m = nx * nz

    @pl.when(pl.program_id(0) == 0)
    def _():
        for i, block in enumerate(blocks):
            at = slice(i * cols, (i + 1) * cols)
            for c in range(comps):
                h, l = parts(block[c].reshape(m, cols))
                rh[c * m : (c + 1) * m, at] = h
                rl[c * m : (c + 1) * m, at] = l

    for i, (e, place) in enumerate(terms):
        g = sender(ids_ref[2], place, groups)
        at = slice(i * cols, (i + 1) * cols)
        for b in range(2):
            lanes = slice(b * cols, (b + 1) * cols)

            @pl.when(g & 1 == b)
            def _():
                th[:, at] = wh_ref[e, g >> 1, :, lanes]
                tl[:, at] = wl_ref[e, g >> 1, :, lanes]

    total = dot3((rh[...], rl[...]), (th[...], tl[...]), dot_t)
    out_ref[...] = base_ref[...] + section_weight * total.reshape(out_ref.shape)


def whole(shape):
    return pl.BlockSpec(shape, lambda *_: (0,) * len(shape))


SMEM = pl.BlockSpec(memory_space=pltpu.SMEM)


def shaped(*shape):
    return jax.ShapeDtypeStruct(shape, F32)


def call(body, flops, moved, **kw):
    return pl.pallas_call(
        body,
        compiler_params=pltpu.CompilerParams(vmem_limit_bytes=VMEM_LIMIT),
        cost_estimate=pl.CostEstimate(flops=int(flops), bytes_accessed=int(moved), transcendentals=0),
        **kw,
    )


SPLIT = ((0, 0), (1, 0))
DIRECT = ((0, 0), (1, 0), (2, 0))


def section(vel, q_old, pressure_guess, shear_shift):
    _, nx, nz, ny = vel.shape
    depth = q_old.shape[2]
    groups = lax.axis_size("yz")
    slabs = lax.axis_size("gx")
    pairs = groups // 2
    cols = ny // groups
    chunks = 2 if cols % 256 == 0 else 1
    cw = cols // chunks
    half = cw // 2
    block_len = cols // 2
    ids = jnp.stack(
        [shear_shift[0], lax.axis_index("gx").astype(jnp.int32), lax.axis_index("yz").astype(jnp.int32)]
    )

    modes = np.arange(ny // 2).reshape(pairs, 2, chunks, half).transpose(2, 0, 1, 3)[:, :, None]
    angle = 2.0 * np.pi / ny * (np.arange(ny).reshape(1, 1, ny, 1, 1) * modes % ny)
    table = np.concatenate([np.cos(angle), -np.sin(angle)], axis=-1) / math.sqrt(ny)
    wh, wl = (jnp.asarray(t) for t in np_parts(table.reshape(chunks, pairs, ny, 2 * cw)))
    kz_np = np.fft.fftfreq(depth) * 2.0 * np.pi
    angle_z = 2.0 * np.pi / depth * (np.arange(depth)[:, None] * np.arange(depth)[None, :] % depth)
    cz = np.cos(angle_z) / math.sqrt(depth)
    sz = np.sin(angle_z) / math.sqrt(depth)
    k1 = kz_np[:, None]
    k2 = viscosity * k1 * k1
    forward = np.concatenate(
        [
            np.concatenate([cz, k1 * sz, -k2 * cz], axis=1),
            np.concatenate([-sz, k1 * cz, k2 * sz], axis=1),
        ],
        axis=0,
    )
    forward = forward.reshape(2 * depth, 3, pairs, 2 * nz).transpose(2, 0, 1, 3)
    fh, fl = np_parts(forward.reshape(pairs, 2 * depth, 6 * nz))
    az = jnp.asarray(np.concatenate([fh, fl, fh], axis=-1))
    bh, bl = (jnp.asarray(t) for t in np_parts(np.concatenate([cz, sz], axis=0)))
    kz = jnp.asarray(kz_np.astype(np.float32)[:, None])

    up = [(i, (i + 1) % slabs) for i in range(slabs)]
    down = [((i + 1) % slabs, i) for i in range(slabs)]
    twins = [(i, i ^ 1) for i in range(groups)]

    def exchange(first, last):
        return lax.ppermute(last, "gx", up), lax.ppermute(first, "gx", down)

    m = nx * nz
    y_flops = 2 * m * ny * ny * 3
    half_bytes = 4 * m * ny
    comp = lambda c: pl.BlockSpec((1, nx, nz, ny), lambda p: (c, 0, 0, 0))

    def fields(kind, c, e, halos=(), direct=False):
        moves, stays = kind != "still", kind != "moving"
        count = {"still": 2, "moving": 3, "full": 4}[kind]
        width = 2 * pairs if direct else 2
        n_out = 2 * stays + moves
        block = lambda f: pl.BlockSpec((1, f, nx, nz, cw), lambda p: (0 if direct else p, 0, 0, 0, 0))
        tables = pl.BlockSpec((1, pairs, ny, 2 * cw), lambda p: (e, 0, 0, 0))
        args, specs = [ids, vel], [SMEM, comp(c)]
        if stays:
            args.append(vel)
            specs.append(comp(2))
        if moves:
            args += [vel, vel, halos[0][0], halos[c][0], halos[0][1], halos[c][1]]
            specs += [comp(0), comp(1)] + [whole((3, nz, ny))] * 4
        args += [wh, wl]
        specs += [tables] * 2
        return call(
            functools.partial(
                y_fields, c=c, e=e, kind=kind, slabs=slabs, chunks=chunks, direct=direct, u_pairs=pairs
            ),
            count * y_flops // chunks,
            count * half_bytes,
            grid=(pairs,),
            in_specs=specs,
            out_specs=[block(n_out)] * width,
            out_shape=[shaped(1 if direct else pairs, n_out, nx, nz, cw)] * width,
            scratch_shapes=[pltpu.VMEM((count * m, ny), BF16)] * 2
            + ([pltpu.VMEM((2, 6, nz, ny), F32)] if moves else []),
        )(*args)

    zb = 2 if nx % 2 == 0 else 1
    plane = (depth, cw)

    def z_part(arrays, layout):
        outs = call(
            functools.partial(z_partial, layout=layout),
            2 * az.size * nx * cw,
            10 * half_bytes // groups,
            grid=(nx // zb,),
            in_specs=[SMEM]
            + [
                pl.BlockSpec((pairs, v.shape[1], zb, nz, cw), lambda x: (0, 0, x, 0, 0))
                for v in arrays
            ]
            + [whole(az.shape)],
            out_specs=[pl.BlockSpec((zb,) + plane, lambda x: (x, 0, 0))] * pairs,
            out_shape=[shaped(nx, *plane)] * pairs,
        )(ids, *arrays, az)
        pieces = [outs[0]]
        for s in range(1, pairs):
            to = [(i, int(across(i // 2, s, pairs)) * 2 + i % 2) for i in range(groups)]
            pieces.append(lax.ppermute(outs[s], "yz", to))
        return pieces

    halos = [exchange(vel[0, :3], vel[0, nx - 3 :])]
    tend = [[None] * 3 for _ in range(chunks)]

    def spread_out(outs):
        got = []
        for s in range(pairs):
            send_s, keep_s = outs[2 * s], outs[2 * s + 1]
            same = [(i, int(across(i // 2, s, pairs)) * 2 + i % 2) for i in range(groups)]
            other = [(i, t ^ 1) for i, t in same]
            got.append(lax.ppermute(keep_s, "yz", same) if s else keep_s)
            got.append(lax.ppermute(send_s, "yz", other))
        return got

    def z_direct(arrays, layout):
        return [
            call(
                functools.partial(z_whole, layout=layout, pairs=pairs),
                2 * az.size * nx * cw,
                10 * half_bytes // groups,
                grid=(nx // zb,),
                in_specs=[SMEM]
                + [
                    pl.BlockSpec((1, v.shape[1], zb, nz, cw), lambda x: (0, 0, x, 0, 0))
                    for v in arrays
                ]
                + [whole(az.shape)],
                out_specs=pl.BlockSpec((zb,) + plane, lambda x: (x, 0, 0)),
                out_shape=shaped(nx, *plane),
            )(ids, *arrays, az)
        ]

    us = fields("still", 0, 0, direct=True)
    later, us = lax.optimization_barrier((vel, us))
    for d in (1, 2):
        halos.append(exchange(later[d, :3], later[d, nx - 3 :]))
    still = {(0, 0): us}
    for c, e in SPLIT:
        us = still.get((c, e)) or fields("still", c, e, direct=True)
        w = fields("moving", c, e, halos, direct=True)
        arrays = spread_out(us) + spread_out(w)
        tend[e][c] = z_direct(arrays, ((1, 0), (0, 1), (0, 0)))
    late = ids
    guess = pressure_guess
    for e in range(chunks):
        for c in range(3):
            if tend[e][c]:
                continue
            direct = (c, e) in DIRECT
            outs = fields("full", c, e, halos, direct)
            if (c, e) == (1, chunks - 1):
                late, guess, outs = lax.optimization_barrier((late, guess, outs))
            if direct:
                arrays = spread_out(outs)
                tend[e][c] = z_direct(arrays, ((0, 2), (0, 1), (0, 0)))
            else:
                sent, kept = outs
                arrays = (kept, lax.ppermute(sent, "yz", twins))
                tend[e][c] = z_part(arrays, ((0, 2), (0, 1), (0, 0)))
    p_low, p_high = exchange(guess[:1], guess[nx - 1 :])

    offset, slab_id, group_id = late[0], late[1], late[2]
    is_low = slab_id == 0
    is_high = slab_id == slabs - 1
    lane = jnp.arange(cw, dtype=jnp.int32)
    sign = jnp.where(lane < half, -1.0, 1.0)
    kys, cks, rdens, rots = [], [], [], []
    for e in range(chunks):
        own = group_id * block_len + e * half + lane % half
        ky = (2.0 * math.pi / ny * own.astype(F32)).reshape(1, cw)
        edge = (
            2.0 * math.pi / ny
            * ((own * offset % ny).astype(F32) + fraction * own.astype(F32))
        )
        cos_e, sin_e = jnp.cos(edge), jnp.sin(edge) * sign
        kys.append(ky)
        cks.append(jnp.where(own == 0, 1.0, 2.0).astype(F32).reshape(1, cw))
        rdens.append(1.0 / (2.0 + ky * ky + kz * kz))
        rots.append(
            jnp.stack(
                [
                    jnp.where(is_low, cos_e, 1.0),
                    jnp.where(is_low, sin_e, 0.0),
                    jnp.where(is_high, cos_e, 1.0),
                    jnp.where(is_high, -sin_e, 0.0),
                ]
            ).astype(F32)
        )

    fb = 2 if nx % 2 == 0 else 1
    one = pl.BlockSpec((fb,) + plane, lambda x: (x, 0, 0))
    three = pl.BlockSpec((3, fb) + plane, lambda x: (0, x, 0, 0))
    packed = (depth, cols)
    q_done = []
    edges = []
    for e in range(chunks):
        edge_of = lambda x: functools.reduce(jnp.add, [piece[x] for piece in tend[e][0]])
        edges.append(exchange(edge_of(0), edge_of(nx - 1)))
    back = []
    for e in range(chunks):
        flat = [piece for c in range(3) for piece in tend[e][c]]
        pieces = tuple(len(tend[e][c]) for c in range(3))
        t_low, t_high = edges[e]
        div, p1, lo, hi = call(
            functools.partial(first_sweep, e=e, chunks=chunks, pieces=pieces),
            2000 * nx * depth * cw,
            2 * half_bytes,
            out_shape=[shaped(nx, *plane)] * 2 + [shaped(2, *plane)] * 2,
        )(*flat, pressure_guess, t_low, t_high, p_low, p_high, rots[e], kys[e], kz, rdens[e])
        lo_halo, hi_halo = exchange(lo, hi)
        last = e == chunks - 1
        earlier = chunks > 1 and last
        out_plane = packed if last else plane
        consts = (p1, div, lo_halo, hi_halo, rots[e], kys[e], kz, rdens[e], cks[e])
        outs = call(
            functools.partial(finish, e=e, chunks=chunks, pieces=pieces, groups=groups),
            2 * 3 * 3 * nx * 2 * depth * depth * cw,
            3 * half_bytes,
            grid=(nx // fb,),
            in_specs=[SMEM]
            + [whole(v.shape) for v in consts]
            + [one] * len(flat)
            + [pl.BlockSpec((3, fb) + packed, lambda x: (0, x, 0, 0)), whole(bh.shape), whole(bl.shape)]
            + ([three, one] if earlier else []),
            out_specs=[
                pl.BlockSpec((3, fb) + out_plane, lambda x: (0, x, 0, 0)),
                pl.BlockSpec((fb,) + out_plane, lambda x: (x, 0, 0)),
            ]
            + [pl.BlockSpec((3, fb, nz, cw), lambda x: (0, x, 0, 0))] * groups,
            out_shape=[shaped(3, nx, *out_plane), shaped(nx, *out_plane)]
            + [shaped(3, nx, nz, cw)] * groups,
            scratch_shapes=[pltpu.VMEM((nx + 2,) + plane, F32), pltpu.VMEM((3,) + plane, F32)],
        )(ids, *consts, *flat, q_old, bh, bl, *q_done)
        q_done = list(outs[:2])
        got = [outs[2]]
        for place in range(1, groups):
            to = [(i, int(partner(i, place, groups))) for i in range(groups)]
            got.append(lax.ppermute(outs[2 + place], "yz", to))
        back.append(got)

    yb = ny // 4
    vel_block = pl.BlockSpec((3, nx, nz, yb), lambda i: (0, 0, 0, i))
    table_block = pl.BlockSpec((chunks, pairs, yb, 2 * cw), lambda i: (0, 0, i, 0))
    batches = [[(e, place) for place in range(groups)] for e in range(chunks - 1)]
    batches += [[(chunks - 1, place) for place in range(groups)]]
    vel_next = vel
    for terms in batches:
        vel_next = call(
            functools.partial(y_inverse, terms=terms, groups=groups),
            3 * y_flops * len(terms) // (chunks * groups),
            6 * half_bytes,
            grid=(ny // yb,),
            in_specs=[SMEM]
            + [whole((3, nx, nz, cw))] * len(terms)
            + [vel_block, table_block, table_block],
            out_specs=vel_block,
            out_shape=jax.ShapeDtypeStruct(vel.shape, F32),
            scratch_shapes=[pltpu.VMEM((3 * m, len(terms) * cw), BF16)] * 2
            + [pltpu.VMEM((yb, len(terms) * cw), BF16)] * 2,
        )(ids, *[back[e][place] for e, place in terms], vel_next, wh, wl)
    return (vel_next, q_done[0], q_done[1])


def solution(mesh):
    placed = (P(None, "gx", "yz", None), P(None, "gx", None, "yz"), P("gx", None, "yz"), P())
    return jax.shard_map(
        section,
        mesh=mesh,
        in_specs=placed,
        out_specs=(P(None, "gx", "yz", None), P(None, "gx", None, "yz"), P("gx", None, "yz")),
        check_vma=False,
    )
```
